32 devices in a mesh: seq: 8 (over z, y), batch: 4 (over x, core).
Axes of the slice: x: 2, y: 2, z: 4, core: 2. Of those that a mesh axis runs over, the one named last changes fastest.
Arguments:
- conv_input: bfloat16 [4096, 8192], P(('batch', 'seq')), parts along dimension 0, may hold values from -6 to 6
- gate_input: bfloat16 [4096, 8192], P(('batch', 'seq')), parts along dimension 0, may hold values from -6 to 6
- conv_weight: bfloat16 [4, 8192], P(None, 'seq'), may hold values from -3 to 3
- conv_bias: bfloat16 [8192], P('seq'), may hold values from -3 to 3
- x_weight: bfloat16 [8192, 288], P('seq'), may hold values from -0.0625 to 0.0625
- dt_gain: float32 [256], replicated, may hold values from 0.5 to 1.5
- dt_weight: bfloat16 [256, 8192], P(None, 'seq'), may hold values from -0.375 to 0.375
- dt_bias: float32 [8192], P('seq'), may hold values from -6.9 to -2.3
- a_log: float32 [16, 8192], P(None, 'seq'), may hold values from 0 to 2.77
- skip: float32 [8192], P('seq'), may hold values from 0.5 to 1.5
Outputs:
- mixed: bfloat16 [4096, 8192], P(('batch', 'seq')), parts along dimension 0
The draws below stay inside these ranges and needn't reach their ends.
There are 4 independent parts, one for each index of `batch`. The reference program is written for one: setup_inputs(seed, part) draws one part's arguments, and reference() takes and returns one part's arrays. A program takes and returns all parts, laid end to end along the dimension named above; an argument that names none is the same for every part. Nothing has to cross between parts.
All inputs are finite; a program needn't handle non-finite values.
Results may differ from the reference program's by a relative error of at most 0.0085.
Values may be sent and summed in bfloat16 or wider, within the bound.
A program may use at most 128 MiB of HBM per device.

```python
import jax
import jax.numpy as jnp
from jax import lax

INNER = 8192
STATE = 16
DT_RANK = 256
CONV = 4
LENGTH = 1024
PROJ = 288


def block_scale(key, extent, pieces, low, top_value):
    def one(axis_at, blocks):
        steps = jax.random.uniform(jax.random.fold_in(jax.random.fold_in(key, 6), axis_at), (blocks,), jnp.float32, low / len(pieces), top_value / len(pieces))
        return jnp.repeat(jnp.exp(steps), extent[axis_at] // blocks).reshape((-1,) + (1,) * (len(extent) - axis_at - 1))

    loudness = one(*pieces[0])
    for cut in pieces[1:]:
        loudness = loudness * one(*cut)
    return loudness


def centred(stream_key, shape, scale, limit, shards=(), kind=jnp.bfloat16):
    drawn = scale * jax.random.normal(stream_key, shape, jnp.float32)
    if shards:
        drawn = drawn * block_scale(stream_key, shape, shards, -0.22, 0.18)
    return jnp.clip(drawn, -limit, limit).astype(kind)


def setup_inputs(seed: int = 0, part: int = 0) -> dict:
    key_list = jax.random.split(jax.random.key(seed), 11)
    part_splits = jax.random.split(jax.random.fold_in(key_list[10], part), 11)
    conv_input = centred(part_splits[0], (LENGTH, INNER), 1.0, 6.0, ((0, 8),))
    gate_input = centred(part_splits[1], (LENGTH, INNER), 1.0, 6.0, ((0, 8),))
    conv_weight = centred(key_list[2], (CONV, INNER), CONV ** -0.5, 3.0, ((1, 8),))
    conv_bias = centred(key_list[3], (INNER,), 0.5, 3.0, ((0, 8),))
    x_weight = centred(key_list[4], (INNER, PROJ), INNER ** -0.5, 0.0625, ((0, 8),))
    dt_gain = jnp.clip(1.0 + 0.1 * jax.random.normal(key_list[5], (DT_RANK,), jnp.float32), 0.5, 1.5)
    dt_weight = centred(key_list[6], (DT_RANK, INNER), DT_RANK ** -0.5, 0.375, ((1, 8),))
    dt_bias = jnp.clip(-6.9 + 4.6000001430511475 * jax.random.uniform(key_list[7], (INNER,), jnp.float32) ** block_scale(key_list[7], (INNER,), ((0, 8),), -0.2, 0.2), -6.9, -2.3)
    a_log = jnp.clip(2.77 * jax.random.uniform(key_list[8], (STATE, INNER), jnp.float32) ** block_scale(key_list[8], (STATE, INNER), ((1, 8),), -0.2, 0.2), 0.0, 2.77)
    skip = jnp.clip(1.0 + 0.1 * jax.random.normal(key_list[9], (INNER,), jnp.float32), 0.5, 1.5)
    return dict(conv_input=conv_input, gate_input=gate_input, conv_weight=conv_weight, conv_bias=conv_bias, x_weight=x_weight, dt_gain=dt_gain, dt_weight=dt_weight, dt_bias=dt_bias, a_log=a_log, skip=skip)


def convolve(inputs, weight, bias):
    rows = inputs.shape[0]
    width = weight.shape[0]
    padded = jnp.concatenate([jnp.zeros((width - 1, inputs.shape[1]), jnp.float32), inputs.astype(jnp.float32)], 0)
    total = bias.astype(jnp.float32)[None, :]
    for tap in range(width):
        total = total + weight[tap].astype(jnp.float32)[None, :] * padded[tap:tap + rows]
    return jax.nn.silu(total).astype(jnp.bfloat16)

def reference(conv_input, gate_input, conv_weight, conv_bias, x_weight, dt_gain, dt_weight, dt_bias, a_log, skip):
    xc = convolve(conv_input, conv_weight, conv_bias)
    proj = jnp.dot(xc, x_weight, preferred_element_type=jnp.float32)
    dt_low = proj[:, :DT_RANK]
    bmat = proj[:, DT_RANK:DT_RANK + STATE]
    cmat = proj[:, DT_RANK + STATE:]
    normed = (dt_low * lax.rsqrt(lax.optimization_barrier(jnp.mean(dt_low * dt_low, axis=1, keepdims=True)) + 1e-06) * dt_gain[None, :]).astype(jnp.bfloat16)
    step = jax.nn.softplus(jnp.dot(normed, dt_weight, preferred_element_type=jnp.float32) + dt_bias[None, :])
    rate = -jnp.exp(a_log)
    xfloat = xc.astype(jnp.float32)

    def advance(state, inputs):
        step_t, x_t, b_t, c_t = inputs
        state = jnp.exp(step_t[None, :] * rate) * state + b_t[:, None] * (step_t * x_t)[None, :]
        return (state, lax.optimization_barrier(jnp.sum(c_t[:, None] * state, axis=0)))
    _, outputs = lax.scan(advance, jnp.zeros((STATE, INNER), jnp.float32), (step, xfloat, bmat, cmat))
    y_out = (outputs + skip[None, :] * xfloat).astype(jnp.bfloat16)
    y_out = lax.optimization_barrier(y_out)
    return (y_out.astype(jnp.float32) * jax.nn.silu(gate_input.astype(jnp.float32))).astype(jnp.bfloat16)
```

```python
import functools
import math

import jax
import jax.numpy as jnp
from jax import lax
from jax.experimental import pallas as pl
from jax.experimental.pallas import tpu as pltpu
from jax.sharding import Mesh
from jax.sharding import PartitionSpec as P

LOG2E = 1.4426950408889634
LN2 = 0.6931471805599453
LANES = 128
ROWS8 = 8
PACK = 16
WIDE = 256
GROUP = 1024
MESH = pl.DeviceIdType.MESH
F32 = jnp.float32
BF16 = jnp.bfloat16


def split_rows(rows, planes):
    half = rows // 2
    if planes == 2:
        private = -(-half // (3 * PACK)) * PACK
        return half, private, half - 2 * private
    return half, half // planes, 0


def padded_rows(rows, planes):
    unit = 2 * PACK * (planes if planes > 2 else 1)
    return -(-rows // unit) * unit


class Gather:
    def __init__(self, sizes, place, which, buf, sems):
        self.A, self.B, self.X = sizes
        self.a, self.b, self.x, self.c = place
        self.w = which
        self.buf = buf
        (self.zs, self.ys, self.xs, self.ds, self.wr, self.xr, self.dr) = sems
        self.half, self.private, self.shared = split_rows(buf.shape[1], self.X)

    def shard(self, i):
        A, B = self.A, self.B
        return lax.rem(self.a - lax.rem(i, A) + A, A) * B + lax.rem(self.b - i // A + B, B)

    def window(self, s, core):
        start = core * self.half + self.x * self.private
        return self.buf.at[s, pl.ds(pl.multiple_of(start, PACK), self.private + self.shared)]

    def own(self, s, core, plane):
        start = core * self.half + plane * (self.private + self.shared)
        return self.buf.at[s, pl.ds(pl.multiple_of(start, PACK), self.private)]

    def copy(self, ref, send, recv, **to):
        return pltpu.make_async_remote_copy(
            src_ref=ref, dst_ref=ref, send_sem=send, recv_sem=recv,
            device_id=to, device_id_type=MESH,
        )

    def along(self, j):
        return self.copy(
            self.window(self.a * self.B + self.b, self.c), self.zs.at[self.w, j], self.wr.at[self.w, j],
            a=lax.rem(self.a + j, self.A),
        )

    def across(self, i, k):
        return self.copy(
            self.window(self.shard(i), self.c), self.ys.at[self.w, k, i],
            self.wr.at[self.w, k * self.A + i], b=lax.rem(self.b + k, self.B),
        )

    def plane(self, i, k):
        return self.copy(
            self.own(self.shard(i), self.c, self.x), self.xs.at[self.w, k, i],
            self.xr.at[self.w, k, i], x=lax.rem(self.x + k, self.X),
        )

    def from_plane(self, i, k):
        ref = self.own(self.shard(i), self.c, lax.rem(self.x - k + self.X, self.X))
        return self.copy(ref, self.xs.at[self.w, k, i], self.xr.at[self.w, k, i], x=self.x)

    def pair(self, i, e, core):
        s = self.shard(i)
        if e == 0:
            ref = self.window(s, core)
        else:
            ref = self.own(s, core, lax.rem(self.x - e + self.X, self.X))
        return self.copy(ref, self.ds.at[self.w, e, i], self.dr.at[self.w, e, i], c=1 - self.c)

    def begin(self):
        for j in range(1, self.A):
            self.along(j).start()
        for k in range(1, self.B):
            self.across(0, k).start()

    def relay(self, i):
        pltpu.make_async_remote_copy(
            src_ref=self.window(self.shard(i), self.c), dst_ref=self.window(self.shard(i), self.c),
            send_sem=self.zs.at[self.w, 0], recv_sem=self.wr.at[self.w, i],
            device_id={"c": self.c}, device_id_type=MESH,
        ).wait_recv()

        @pl.when(i < self.A)
        def _():
            for k in range(1, self.B):
                self.across(i, k).start()

        for k in range(1, self.X):
            self.plane(i, k).start()
        self.pair(i, 0, self.c).start()

    def relay_plane(self, i):
        for k in range(1, self.X):
            self.from_plane(i, k).wait_recv()
            self.pair(i, k, self.c).start()

    def ready(self, i):
        for e in range(self.X):
            self.pair(i, e, 1 - self.c).wait_recv()

    def drain(self):
        for j in range(1, self.A):
            self.along(j).wait_send()
        for k in range(1, self.B):
            lax.fori_loop(0, self.A, lambda i, _: (self.across(i, k).wait_send(), 0)[1], 0)

        def one(i, _):
            for k in range(1, self.X):
                self.plane(i, k).wait_send()
            for e in range(self.X):
                self.pair(i, e, self.c).wait_send()
            return 0

        lax.fori_loop(1, self.A * self.B, one, 0)


def scan_tokens(st, dr, bx, rate, hidden, tokens, unroll, each=None):
    tiles = GROUP // LANES
    rates = [[rate[8 * k : 8 * k + 8, LANES * j : LANES * j + LANES] for j in range(tiles)] for k in range(2)]

    def body(i, carry):
        h = [list(carry[:tiles]), list(carry[tiles:])]
        for u in range(unroll):
            at = pl.multiple_of((i * unroll + u) * 16, 16)
            b = [bx[pl.ds(at + 8 * k, 8), :] for k in range(2)]
            block = i * (unroll // ROWS8) + u // ROWS8
            row = slice(u % ROWS8, u % ROWS8 + 1)
            for j in range(tiles):
                cols = slice(LANES * j, LANES * j + LANES)
                s = jnp.broadcast_to(st[block, row, cols], (ROWS8, LANES))
                d = jnp.broadcast_to(dr[block, row, cols], (ROWS8, LANES))
                for k in range(2):
                    h[k][j] = jnp.exp2(s * rates[k][j]) * h[k][j] + b[k] * d
                if each is not None:
                    each(i, u, j, h[0][j], h[1][j])
        if each is not None:
            each(i, None, None, None, None)
        return tuple(h[0]) + tuple(h[1])

    return lax.fori_loop(0, tokens // unroll, body, hidden)


def mixer_kernel(
    sizes, states,
    x_hbm, g_hbm, xw_hbm, dtw_hbm, pk_hbm, gain_ref,
    out_hbm,
    xv, gv, xwv, dtv, pkv, halo, cp, w1, w2, acc, acc2, nm, bx, cblk, st, dr, rt, hs,
    eb, rb, sb, h0b,
    lsem, osem, hsem, csem_s, csem_r,
    zs, ys, xs, ds, wr, xr, dr_sem,
    es, er, bs, br,
):
    A, B, X = sizes
    D = A * B
    tokens, inner = xv.shape
    shard = pkv.shape[1]
    nb = shard // WIDE
    rank = gain_ref.shape[1]
    extra = 2 * states
    groups = inner // GROUP
    span = rank + 3 * PACK
    a, b, x, c = (lax.axis_index(n) for n in ("a", "b", "x", "c"))
    me = a * B + b
    place = (a, b, x, c)
    sems = (zs, ys, xs, ds, wr, xr, dr_sem)

    loads = [
        pltpu.make_async_copy(src, dst, lsem.at[n])
        for n, (src, dst) in enumerate(((pk_hbm, pkv), (xw_hbm, xwv), (dtw_hbm, dtv), (x_hbm, xv), (g_hbm, gv)))
    ]
    for load in loads:
        load.start()

    barrier = pltpu.get_barrier_semaphore()
    for r in range(1, D):
        other = lax.rem(me + r, D)
        pl.semaphore_signal(
            barrier, inc=1, device_id={"a": other // B, "b": lax.rem(other, B)}, device_id_type=MESH
        )
    for k in range(1, X):
        pl.semaphore_signal(barrier, inc=1, device_id={"x": lax.rem(x + k, X)}, device_id_type=MESH)
    pl.semaphore_signal(barrier, inc=1, device_id={"c": 1 - c}, device_id_type=MESH)

    loads[0].wait()
    for j in range(nb):
        cols = slice(WIDE * j, WIDE * j + WIDE)
        cp[me, j] = pkv[0:ROWS8, cols]
        rate = -jnp.exp(pkv[ROWS8 : ROWS8 + states, cols]) * LOG2E
        high = rate.astype(BF16)
        base = j * span + rank
        w2[me, base : base + states, :] = high
        w2[me, base + PACK : base + PACK + states, :] = (rate - high.astype(F32)).astype(BF16)
        two = pkv[5:7, cols]
        top = two.astype(BF16).astype(F32)
        w2[me, base + 2 * PACK : base + 3 * PACK, :] = jnp.concatenate(
            [top, two - top, jnp.zeros((PACK - 4, WIDE), F32)], 0
        ).astype(BF16)
    loads[1].wait()
    w1[me, 0:shard, :] = xwv[:, 0:rank]
    pick = (
        lax.broadcasted_iota(jnp.int32, (extra, rank + extra), 1)
        == lax.broadcasted_iota(jnp.int32, (extra, rank + extra), 0) + rank
    ).astype(BF16)
    for j in range(nb):
        turned = lax.dot_general(
            pick, xwv[WIDE * j : WIDE * j + WIDE, :], (((1,), (1,)), ((), ())), preferred_element_type=F32
        )
        w1[me, shard + extra * j : shard + extra * j + extra, :] = turned.astype(BF16)
    pl.semaphore_wait(barrier, D - 1 + X - 1 + 1)

    def pack_copy(r):
        other = lax.rem(me + r, D)
        return pltpu.make_async_remote_copy(
            src_ref=cp.at[me], dst_ref=cp.at[me], send_sem=csem_s.at[r], recv_sem=csem_r.at[r],
            device_id={"a": other // B, "b": lax.rem(other, B)}, device_id_type=MESH,
        )

    after = lax.rem(me + 1, D)
    halo_copy = pltpu.make_async_remote_copy(
        src_ref=x_hbm.at[pl.ds(tokens - ROWS8, ROWS8)], dst_ref=halo, send_sem=hsem.at[0], recv_sem=hsem.at[1],
        device_id={"a": after // B, "b": lax.rem(after, B)}, device_id_type=MESH,
    )
    for r in range(1, D):
        pack_copy(r).start()
    halo_copy.start()

    first = Gather(sizes, place, 0, w1, sems)
    second = Gather(sizes, place, 1, w2, sems)
    first.begin()

    loads[2].wait()
    for j in range(nb):
        w2[me, j * span : j * span + rank, :] = dtv[:, WIDE * j : WIDE * j + WIDE]

    for r in range(1, D):
        other = lax.rem(me - r + D, D)
        pltpu.make_async_remote_copy(
            src_ref=cp.at[other], dst_ref=cp.at[other], send_sem=csem_s.at[r], recv_sem=csem_r.at[r],
            device_id={"c": c}, device_id_type=MESH,
        ).wait_recv()
    halo_copy.wait_recv()
    loads[3].wait()
    lead = (me > 0).astype(F32)

    def convolve(q, _):
        cols = pl.ds(pl.multiple_of(q * WIDE, WIDE), WIDE)
        taps = cp.at[q // nb, lax.rem(q, nb)]
        cur = xv[:, cols].astype(F32)
        ext = jnp.concatenate([halo[:, cols].astype(F32) * lead, cur], 0)
        total = taps[4:5, :] + taps[3:4, :] * cur
        for tap in range(3):
            low = ROWS8 - 3 + tap
            total = total + taps[tap : tap + 1, :] * ext[low : low + tokens]
        xv[:, cols] = (total / (1.0 + jnp.exp(-total))).astype(BF16)
        return 0

    lax.fori_loop(0, inner // WIDE, convolve, 0)

    def relay_first(i, _):
        first.relay(i)

        @pl.when(i > 1)
        def _():
            first.relay_plane(i - 1)

        return 0

    lax.fori_loop(1, A, relay_first, 0)
    second.begin()
    lax.fori_loop(A, D, relay_first, 0)
    first.relay_plane(D - 1)

    acc[...] = jnp.zeros_like(acc)
    acc2[...] = jnp.zeros_like(acc2)

    def project(i, _):
        @pl.when(i > 0)
        def _():
            first.ready(i)

        s = first.shard(i)
        base = pl.multiple_of(s * shard, WIDE)
        acc[...] += jnp.dot(xv[:, pl.ds(base, shard)], w1[s, 0:shard, :], preferred_element_type=F32)
        for j in range(nb):
            acc2[...] += lax.dot_general(
                xv[:, pl.ds(base + WIDE * j, WIDE)], w1[s, shard + extra * j : shard + extra * j + extra, :],
                (((1,), (1,)), ((), ())), preferred_element_type=F32,
            )
        return 0

    lax.fori_loop(0, D, project, 0)

    low = acc[...]
    nm[...] = (
        low * lax.rsqrt(jnp.mean(low * low, axis=1, keepdims=True) + 1e-06) * gain_ref[...]
    ).astype(BF16)
    bc = acc2[...]
    for n in range(states):
        bx[pl.ds(n, tokens, stride=states), :] = jnp.broadcast_to(bc[:, n : n + 1], (tokens, LANES))
    lane = lax.broadcasted_iota(jnp.int32, (extra, PACK * states), 1)
    spread = (
        lax.broadcasted_iota(jnp.int32, (extra, PACK * states), 0) == states + lax.rem(lane, states)
    ).astype(BF16)
    tiled = jnp.dot(bc.astype(BF16), spread, preferred_element_type=F32)
    slot = lax.broadcasted_iota(jnp.int32, tiled.shape, 1) // states
    turn = lax.rem(lax.broadcasted_iota(jnp.int32, tiled.shape, 0), PACK)
    cblk[...] = jnp.where(slot == turn, tiled, 0.0).astype(BF16)

    tiles = GROUP // LANES
    blocks = GROUP // WIDE
    local_order = groups == D

    def group_at(i):
        return second.shard(i) if local_order else i

    def to_combiner(g):
        return pltpu.make_async_remote_copy(
            src_ref=eb.at[g], dst_ref=rb.at[me], send_sem=es.at[g], recv_sem=er.at[me],
            device_id={"a": g // B, "b": lax.rem(g, B)}, device_id_type=MESH,
        )

    def pass_one(i, _):
        if local_order:
            @pl.when(i + 2 < D)
            def _():
                second.relay(i + 2)

            @pl.when(i + 1 < D)
            def _():
                second.relay_plane(i + 1)

            @pl.when(i > 0)
            def _():
                second.ready(i)

        g = group_at(i)
        sums = []
        for q in range(blocks):
            cb = g * blocks + q
            s, j = cb // nb, lax.rem(cb, nb)
            cols = pl.ds(pl.multiple_of(cb * WIDE, WIDE), WIDE)
            base = pl.multiple_of(j * span, PACK)
            rows = lambda n: pl.ds(pl.multiple_of(base + rank + n * PACK, PACK), PACK)
            misc = w2[s, rows(2), :].astype(F32)
            rt[g, :, WIDE * q : WIDE * q + WIDE] = w2[s, rows(0), :].astype(F32) + w2[s, rows(1), :].astype(F32)
            raw = jnp.dot(nm[...], w2[s, pl.ds(base, rank), :], preferred_element_type=F32)
            raw = raw + (misc[0:1] + misc[2:3])
            small = jnp.exp2(jnp.abs(raw) * -LOG2E)
            step = jnp.maximum(raw, 0.0) + LN2 * jnp.log2(1.0 + small)
            st[:, :, cols] = step.reshape(tokens // ROWS8, ROWS8, WIDE)
            dr[:, :, cols] = (step * xv[:, cols].astype(F32)).reshape(tokens // ROWS8, ROWS8, WIDE)
            total = jnp.sum(step, axis=0, keepdims=True)
            sums += [total[:, :LANES], total[:, LANES:]]
        view = pl.ds(pl.multiple_of(g * GROUP, GROUP), GROUP)
        zero = jnp.zeros((ROWS8, LANES), F32)
        h = scan_tokens(
            st.at[:, :, view], dr.at[:, :, view], bx, rt.at[g], (zero,) * (2 * tiles), tokens, ROWS8
        )
        for j in range(tiles):
            eb[g, 16 * j : 16 * j + 16, :] = jnp.concatenate([h[j], h[tiles + j]], 0).astype(BF16)
        sums = jnp.concatenate(sums, 0)
        top = sums.astype(BF16).astype(F32)
        eb[g, 16 * tiles : 16 * tiles + 16, :] = jnp.concatenate([top, sums - top], 0).astype(BF16)

        @pl.when(g != me)
        def _():
            to_combiner(g).start()

        @pl.when(g == me)
        def _():
            rb[me] = eb[me]

        return 0

    if local_order:
        second.relay(1)
    else:
        def settle(i, _):
            second.relay(i)
            second.relay_plane(i)
            second.ready(i)
            return 0

        lax.fori_loop(1, D, settle, 0)
    lax.fori_loop(0, groups, pass_one, 0)

    def to_owner(k):
        return pltpu.make_async_remote_copy(
            src_ref=sb.at[k], dst_ref=h0b.at[me], send_sem=bs.at[k], recv_sem=br.at[me],
            device_id={"a": k // B, "b": lax.rem(k, B)}, device_id_type=MESH,
        )

    def arrival(k):
        return pltpu.make_async_remote_copy(
            src_ref=rb.at[k], dst_ref=rb.at[k], send_sem=es.at[0], recv_sem=er.at[k],
            device_id={"c": c}, device_id_type=MESH,
        )

    @pl.when(me < groups)
    def _():
        def combine(k, start):
            @pl.when(k != me)
            def _():
                arrival(k).wait_recv()

            now = []
            both = rb[k, 16 * tiles : 16 * tiles + 16, :].astype(F32)
            sums = both[0:8] + both[8:16]
            for j in range(tiles):
                sb[k, 16 * j : 16 * j + 16, :] = start[j].astype(BF16)
                decay = jnp.exp2(sums[j : j + 1, :] * rt[me, :, LANES * j : LANES * j + LANES])
                now.append(decay * start[j] + rb[k, 16 * j : 16 * j + 16, :].astype(F32))

            @pl.when(k != me)
            def _():
                to_owner(k).start()

            @pl.when(k == me)
            def _():
                h0b[me] = sb[me]

            return tuple(now)

        lax.fori_loop(0, D, combine, (jnp.zeros((16, LANES), F32),) * tiles)

    loads[4].wait()

    def start_of(g):
        return pltpu.make_async_remote_copy(
            src_ref=h0b.at[g], dst_ref=h0b.at[g], send_sem=bs.at[0], recv_sem=br.at[g],
            device_id={"c": c}, device_id_type=MESH,
        )

    def put(g):
        view = pl.ds(pl.multiple_of(g * GROUP, GROUP), GROUP)
        return pltpu.make_async_copy(gv.at[:, view], out_hbm.at[:, view], osem.at[g])

    def pass_two(g, _):
        @pl.when(g != me)
        def _():
            start_of(g).wait_recv()

        first_state = [h0b[g, 16 * j : 16 * j + 16, :].astype(F32) for j in range(tiles)]
        h = tuple(v[:8] for v in first_state) + tuple(v[8:] for v in first_state)
        view = pl.ds(pl.multiple_of(g * GROUP, GROUP), GROUP)
        xg, gg = xv.at[:, view], gv.at[:, view]
        direct = []
        for q in range(blocks):
            cb = g * blocks + q
            s, j = cb // nb, lax.rem(cb, nb)
            misc = w2[s, pl.ds(pl.multiple_of(j * span + rank + 2 * PACK, PACK), PACK), :].astype(F32)
            direct.append(misc[1:2] + misc[3:4])

        def each(i, u, j, lo, hi):
            if u is not None:
                hs[16 * u : 16 * u + 16, LANES * j : LANES * j + LANES] = jnp.concatenate([lo, hi], 0).astype(BF16)
                return
            rows = pl.ds(pl.multiple_of(i * PACK, PACK), PACK)
            for q in range(blocks):
                cols = slice(WIDE * q, WIDE * q + WIDE)
                y = jnp.dot(cblk[rows, :], hs[:, cols], preferred_element_type=F32)
                y = y + direct[q] * xg[rows, cols].astype(F32)
                gate = gg[rows, cols].astype(F32)
                gg[rows, cols] = (y * gate / (1.0 + jnp.exp(-gate))).astype(BF16)

        scan_tokens(st.at[:, :, view], dr.at[:, :, view], bx, rt.at[g], h, tokens, PACK, each)
        put(g).start()
        return 0

    lax.fori_loop(0, groups, pass_two, 0)

    def finish(g, _):
        put(g).wait()

        @pl.when(g != me)
        def _():
            to_combiner(g).wait_send()

        return 0

    lax.fori_loop(0, groups, finish, 0)

    @pl.when(me < groups)
    def _():
        def sent(k, _):
            @pl.when(k != me)
            def _():
                to_owner(k).wait_send()

            return 0

        lax.fori_loop(0, D, sent, 0)

    for r in range(1, D):
        pack_copy(r).wait_send()
    halo_copy.wait_send()
    first.drain()
    second.drain()


def local(sizes, conv_input, gate_input, conv_weight, conv_bias, x_weight, dt_gain, dt_weight, dt_bias, a_log, skip):
    A, B, X = sizes
    D = A * B
    tokens, inner = conv_input.shape
    rank, shard = dt_weight.shape
    states = a_log.shape[0]
    extra = x_weight.shape[1] - rank
    nb = shard // WIDE
    groups = inner // GROUP
    pack = jnp.concatenate(
        [conv_weight.astype(F32), conv_bias.astype(F32)[None], dt_bias[None], skip[None],
         jnp.zeros((1, shard), F32), a_log], 0
    )
    r1 = padded_rows(shard + extra * nb, X)
    r2 = padded_rows((rank + 3 * PACK) * nb, X)
    tiles = GROUP // LANES
    packet = 16 * tiles + 16
    hbm = pl.BlockSpec(memory_space=pl.ANY)
    vmem = pl.BlockSpec(memory_space=pltpu.VMEM)
    dma = pltpu.SemaphoreType.DMA
    return pl.pallas_call(
        functools.partial(mixer_kernel, sizes, states),
        in_specs=[hbm] * 5 + [vmem],
        out_specs=hbm,
        out_shape=jax.ShapeDtypeStruct((tokens, inner), BF16),
        scratch_shapes=[
            pltpu.VMEM((tokens, inner), BF16),
            pltpu.VMEM((tokens, inner), BF16),
            pltpu.VMEM(x_weight.shape, BF16),
            pltpu.VMEM(dt_weight.shape, BF16),
            pltpu.VMEM(pack.shape, F32),
            pltpu.VMEM((ROWS8, inner), BF16),
            pltpu.VMEM((D, nb, ROWS8, WIDE), F32),
            pltpu.VMEM((D, r1, WIDE), BF16),
            pltpu.VMEM((D, r2, WIDE), BF16),
            pltpu.VMEM((tokens, rank), F32),
            pltpu.VMEM((tokens, extra), F32),
            pltpu.VMEM((tokens, rank), BF16),
            pltpu.VMEM((tokens * states, LANES), F32),
            pltpu.VMEM((tokens, PACK * states), BF16),
            pltpu.VMEM((tokens // ROWS8, ROWS8, inner), F32),
            pltpu.VMEM((tokens // ROWS8, ROWS8, inner), F32),
            pltpu.VMEM((groups, states, GROUP), F32),
            pltpu.VMEM((PACK * states, GROUP), BF16),
            pltpu.VMEM((groups, packet, LANES), BF16),
            pltpu.VMEM((D, packet, LANES), BF16),
            pltpu.VMEM((D, 16 * tiles, LANES), BF16),
            pltpu.VMEM((groups, 16 * tiles, LANES), BF16),
            dma((5,)), dma((groups,)), dma((2,)), dma((D,)), dma((D,)),
            dma((2, A)), dma((2, B, A)), dma((2, X, D)), dma((2, X, D)),
            dma((2, D)), dma((2, X, D)), dma((2, X, D)),
            dma((groups,)), dma((D,)), dma((D,)), dma((groups,)),
        ],
        compiler_params=pltpu.CompilerParams(
            collective_id=0, has_side_effects=True, vmem_limit_bytes=60 * 1024 * 1024
        ),
        name="mixer",
    )(conv_input, gate_input, x_weight, dt_weight, pack, dt_gain[None, :])


def solution(mesh):
    seq, batch = mesh.shape["seq"], mesh.shape["batch"]
    cores = 2
    A = math.gcd(seq, batch)
    B, X = seq // A, batch // cores
    grid = Mesh(mesh.devices.reshape(A, B, X, cores), ("a", "b", "x", "c"))
    seqs = ("a", "b")
    rows = P(("x", "c", "a", "b"), None)
    return jax.shard_map(
        functools.partial(local, (A, B, X)),
        mesh=grid,
        in_specs=(
            rows, rows, P(None, seqs), P(seqs), P(seqs, None), P(), P(None, seqs), P(seqs), P(None, seqs), P(seqs),
        ),
        out_specs=rows,
        check_vma=False,
    )
```

```python
import functools
import math

import jax
import jax.numpy as jnp
from jax import lax
from jax.experimental import pallas as pl
from jax.experimental.pallas import tpu as pltpu
from jax.sharding import Mesh
from jax.sharding import PartitionSpec as P

LOG2E = 1.4426950408889634
LN2 = 0.6931471805599453
LANES = 128
ROWS8 = 8
PACK = 16
WIDE = 256
GROUP = 1024
STEP = 16
TILES = 4
PITCH = 9
MESH = pl.DeviceIdType.MESH
F32 = jnp.float32
BF16 = jnp.bfloat16


def split_rows(rows, planes):
    half = rows // 2
    if planes == 2:
        private = -(-half // (3 * PACK)) * PACK
        return half, private, half - 2 * private
    return half, half // planes, 0


def padded_rows(rows, planes):
    unit = 2 * PACK * (planes if planes > 2 else 1)
    return -(-rows // unit) * unit


def column(a, i, size):
    turn = lax.rem(i, 2)
    inner = a + (1 - 2 * turn) * ((i + 1) // 2)
    outer = jnp.where(2 * a < size - 1, i, size - 1 - i)
    return jnp.where(i <= 2 * jnp.minimum(a, size - 1 - a), inner, outer)


class Gather:
    def __init__(self, sizes, place, which, buf, sems, small=None, small_sems=None):
        self.A, self.B, self.X = sizes
        self.a, self.b, self.x, self.c = place
        self.w = which
        self.buf = buf
        (self.zs, self.ys, self.xs, self.ds, self.wr, self.xr, self.dr) = sems
        self.small = small
        self.small_sems = small_sems
        self.half, self.private, self.shared = split_rows(buf.shape[1], self.X)

    def shard(self, i):
        a = column(self.a, lax.rem(i, self.A), self.A)
        return a * self.B + lax.rem(self.b - i // self.A + self.B, self.B)

    def window(self, s, core):
        start = core * self.half + self.x * self.private
        return self.buf.at[s, pl.ds(pl.multiple_of(start, PACK), self.private + self.shared)]

    def own(self, s, core, plane):
        start = core * self.half + plane * (self.private + self.shared)
        return self.buf.at[s, pl.ds(pl.multiple_of(start, PACK), self.private)]

    def copy(self, ref, send, recv, **to):
        return pltpu.make_async_remote_copy(
            src_ref=ref, dst_ref=ref, send_sem=send, recv_sem=recv,
            device_id=to, device_id_type=MESH,
        )

    def along(self, p, way):
        s = p * self.B + self.b
        to = self.a + 1 - 2 * way
        out = []
        if self.small is not None:
            zs, _, wr = self.small_sems
            out.append(self.copy(self.small.at[s], zs.at[way, p], wr.at[s], a=to))
        out.append(self.copy(self.window(s, self.c), self.zs.at[self.w, way, p], self.wr.at[self.w, s], a=to))
        return out

    def across(self, p, k):
        s = p * self.B + self.b
        to = lax.rem(self.b + k, self.B)
        out = []
        if self.small is not None:
            _, ys, wr = self.small_sems
            out.append(self.copy(self.small.at[s], ys.at[k, p], wr.at[s], b=to))
        out.append(self.copy(self.window(s, self.c), self.ys.at[self.w, k, p], self.wr.at[self.w, s], b=to))
        return out

    def plane(self, s, k):
        return self.copy(
            self.own(s, self.c, self.x), self.xs.at[self.w, k, s],
            self.xr.at[self.w, k, s], x=lax.rem(self.x + k, self.X),
        )

    def from_plane(self, s, k):
        ref = self.own(s, self.c, lax.rem(self.x - k + self.X, self.X))
        return self.copy(ref, self.xs.at[self.w, k, s], self.xr.at[self.w, k, s], x=self.x)

    def pair(self, s, e, core):
        if e == 0:
            ref = self.window(s, core)
        else:
            ref = self.own(s, core, lax.rem(self.x - e + self.X, self.X))
        return self.copy(ref, self.ds.at[self.w, e, s], self.dr.at[self.w, e, s], c=1 - self.c)

    def sends(self, p, right, left, run):
        @pl.when(right & (self.a + 1 < self.A))
        def _():
            run(self.along(p, 0))

        @pl.when(left & (self.a > 0))
        def _():
            run(self.along(p, 1))

    @staticmethod
    def start(copies):
        for copy in copies:
            copy.start()

    @staticmethod
    def sent(copies):
        for copy in copies:
            copy.wait_send()

    def begin(self):
        self.sends(self.a, self.a >= 0, self.a >= 0, self.start)
        for k in range(1, self.B):
            self.start(self.across(self.a, k))

    def relay(self, i):
        s = self.shard(i)
        p = s // self.B
        if self.small is not None:
            zs, _, wr = self.small_sems
            self.copy(self.small.at[s], zs.at[0, 0], wr.at[s], c=self.c).wait_recv()
        self.copy(self.window(s, self.c), self.zs.at[self.w, 0, 0], self.wr.at[self.w, s], c=self.c).wait_recv()

        @pl.when(i < self.A)
        def _():
            self.sends(p, p < self.a, p > self.a, self.start)
            for k in range(1, self.B):
                self.start(self.across(p, k))

        for k in range(1, self.X):
            self.plane(s, k).start()
        self.pair(s, 0, self.c).start()

    def relay_plane(self, i):
        s = self.shard(i)
        for k in range(1, self.X):
            self.from_plane(s, k).wait_recv()
            self.pair(s, k, self.c).start()

    def ready(self, i):
        s = self.shard(i)
        for e in range(self.X):
            self.pair(s, e, 1 - self.c).wait_recv()

    def drain(self):
        def line(p, _):
            self.sends(p, p <= self.a, p >= self.a, self.sent)
            for k in range(1, self.B):
                self.sent(self.across(p, k))
            return 0

        lax.fori_loop(0, self.A, line, 0)

        def one(i, _):
            s = self.shard(i)
            for k in range(1, self.X):
                self.plane(s, k).wait_send()
            for e in range(self.X):
                self.pair(s, e, self.c).wait_send()
            return 0

        lax.fori_loop(1, self.A * self.B, one, 0)


def scan_tokens(st, dr, bx, rate, hidden, tokens, tiles, each=None):
    rates = [[rate[8 * k : 8 * k + 8, cols] for cols in tiles] for k in range(2)]
    count = len(tiles)

    def body(i, carry):
        h = [list(carry[:count]), list(carry[count:])]
        for u in range(STEP):
            at = pl.multiple_of((i * STEP + u) * 16, 16)
            b = [bx[pl.ds(at + 8 * k, 8), :] for k in range(2)]
            block = i * (STEP // ROWS8) + u // ROWS8
            row = slice(u % ROWS8, u % ROWS8 + 1)
            for j, cols in enumerate(tiles):
                s = jnp.broadcast_to(st[block, row, cols], (ROWS8, LANES))
                d = jnp.broadcast_to(dr[block, row, cols], (ROWS8, LANES))
                for k in range(2):
                    h[k][j] = jnp.exp2(s * rates[k][j]) * h[k][j] + b[k] * d
            if each is not None:
                each(i, u, at, h)
        return tuple(h[0]) + tuple(h[1])

    return lax.fori_loop(0, tokens // STEP, body, hidden)


def silu(v):
    half = 0.5 * v
    return half + half * jnp.tanh(half)


def mixer_kernel(
    sizes, states,
    x_hbm, g_hbm, xw_hbm, dtw_hbm, cw_ref, cb_ref, db_ref, sk_ref, al_ref, gain_ref,
    out_hbm,
    xv, gv, xwv, dtv, halo, cp, w1, w2, acc, nm, bx, cx, st, dr, rt, zb,
    eb, rb, sb, h0b,
    lsem, osem, hsem, cz, cy, cr,
    zs, ys, xs, ds, wr, xr, dr_sem,
    es, er, bs, br,
):
    A, B, X = sizes
    D = A * B
    tokens, inner = xv.shape
    wide, shard = xwv.shape
    nb = shard // WIDE
    rank = gain_ref.shape[1]
    taps = cw_ref.shape[0]
    groups = inner // GROUP
    span = rank + 3 * PACK
    a, b, x, c = (lax.axis_index(n) for n in ("a", "b", "x", "c"))
    me = a * B + b
    place = (a, b, x, c)
    sems = (zs, ys, xs, ds, wr, xr, dr_sem)

    loads = [
        pltpu.make_async_copy(src, dst, lsem.at[n])
        for n, (src, dst) in enumerate(((xw_hbm, xwv), (dtw_hbm, dtv), (x_hbm, xv), (g_hbm, gv)))
    ]
    for load in loads:
        load.start()

    barrier = pltpu.get_barrier_semaphore()
    for r in range(1, D):
        other = lax.rem(me + r, D)
        pl.semaphore_signal(
            barrier, inc=1, device_id={"a": other // B, "b": lax.rem(other, B)}, device_id_type=MESH
        )
    for k in range(1, X):
        pl.semaphore_signal(barrier, inc=1, device_id={"x": lax.rem(x + k, X)}, device_id_type=MESH)
    pl.semaphore_signal(barrier, inc=1, device_id={"c": 1 - c}, device_id_type=MESH)

    rows = [cw_ref[...].astype(F32), cb_ref[...].astype(F32)]
    fill = cp.shape[1] - (taps + 1) * nb
    pieces = [r[:, WIDE * j : WIDE * j + WIDE] for j in range(nb) for r in rows]
    cp[me] = jnp.concatenate(pieces + [jnp.zeros((fill, WIDE), F32)], 0).astype(BF16)
    loads[0].wait()
    for j in range(nb):
        w1[me, wide * j : wide * j + wide, :] = xwv[:, WIDE * j : WIDE * j + WIDE]
    pl.semaphore_wait(barrier, D - 1 + X - 1 + 1)

    after = lax.rem(me + 1, D)
    halo_copy = pltpu.make_async_remote_copy(
        src_ref=x_hbm.at[pl.ds(tokens - ROWS8, ROWS8)], dst_ref=halo, send_sem=hsem.at[0], recv_sem=hsem.at[1],
        device_id={"a": after // B, "b": lax.rem(after, B)}, device_id_type=MESH,
    )
    first = Gather(sizes, place, 0, w1, sems, cp, (cz, cy, cr))
    second = Gather(sizes, place, 1, w2, sems)
    first.begin()
    halo_copy.start()

    for j in range(nb):
        cols = slice(WIDE * j, WIDE * j + WIDE)
        rate = -jnp.exp(al_ref[:, cols]) * LOG2E
        high = rate.astype(BF16)
        base = j * span + rank
        w2[me, base : base + states, :] = high
        w2[me, base + PACK : base + PACK + states, :] = (rate - high.astype(F32)).astype(BF16)
        two = jnp.concatenate([db_ref[:, cols], sk_ref[:, cols]], 0)
        top = two.astype(BF16).astype(F32)
        w2[me, base + 2 * PACK : base + 3 * PACK, :] = jnp.concatenate(
            [top, two - top, jnp.zeros((PACK - 4, WIDE), F32)], 0
        ).astype(BF16)
    loads[1].wait()
    for j in range(nb):
        w2[me, j * span : j * span + rank, :] = dtv[:, WIDE * j : WIDE * j + WIDE]
    loads[2].wait()
    acc[...] = jnp.zeros_like(acc)
    halo_copy.wait_recv()
    lead = (me > 0).astype(F32)

    def convolve(i):
        s = first.shard(i)
        weight = cp[s].astype(F32)
        for j in range(nb):
            cols = pl.ds(pl.multiple_of(s * shard + WIDE * j, WIDE), WIDE)
            row = lambda n: weight[(taps + 1) * j + n : (taps + 1) * j + n + 1]
            cur = xv[:, cols].astype(F32)
            ext = jnp.concatenate([halo[:, cols].astype(F32) * lead, cur], 0)
            total = row(taps) + row(taps - 1) * cur
            for tap in range(taps - 1):
                low = ROWS8 - taps + 1 + tap
                total = total + row(tap) * ext[low : low + tokens]
            xv[:, cols] = silu(total).astype(BF16)

    def project(i):
        s = first.shard(i)
        total = acc[...]
        for j in range(nb):
            cols = pl.ds(pl.multiple_of(s * shard + WIDE * j, WIDE), WIDE)
            total = total + lax.dot_general(
                xv[:, cols], w1[s, wide * j : wide * j + wide, :], (((1,), (1,)), ((), ())), preferred_element_type=F32
            )
        acc[...] = total

    def step_first(i, _):
        @pl.when(i > 0)
        def _():
            first.relay(i)

        @pl.when(i > 1)
        def _():
            first.relay_plane(i - 1)

        convolve(i)

        @pl.when(i > 2)
        def _():
            first.ready(i - 2)

        @pl.when(i > 1)
        def _():
            project(i - 2)

        return 0

    with jax.named_scope("w1a"):
        lax.fori_loop(0, A, step_first, 0)
    second.begin()
    with jax.named_scope("w1b"):
        lax.fori_loop(A, D, step_first, 0)
    with jax.named_scope("w1c"):
        first.relay_plane(D - 1)
        first.ready(D - 2)
        project(D - 2)
        first.ready(D - 1)
        project(D - 1)

    with jax.named_scope("norm"):
        low = acc[:, :rank]
        nm[...] = (
            low * lax.rsqrt(jnp.mean(low * low, axis=1, keepdims=True) + 1e-06) * gain_ref[...]
        ).astype(BF16)
        bc = acc[:, rank:]
        for n in range(states):
            at = pl.ds(n, tokens, stride=states)
            bx[at, :] = jnp.broadcast_to(bc[:, n : n + 1], (tokens, LANES))
            cx[at, :] = jnp.broadcast_to(bc[:, states + n : states + n + 1], (tokens, LANES))

    tiles = GROUP // LANES
    blocks = GROUP // WIDE
    local_order = groups == D

    def strips(part):
        return [slice(LANES * j, LANES * j + LANES) for j in range(part, part + TILES)]

    def group_at(i):
        return second.shard(i) if local_order else i

    def to_combiner(g):
        return pltpu.make_async_remote_copy(
            src_ref=eb.at[g], dst_ref=rb.at[me], send_sem=es.at[g], recv_sem=er.at[me],
            device_id={"a": g // B, "b": lax.rem(g, B)}, device_id_type=MESH,
        )

    def pass_one(i, _):
        if local_order:
            @pl.when(i + 2 < D)
            def _():
                second.relay(i + 2)

            @pl.when(i + 1 < D)
            def _():
                second.relay_plane(i + 1)

            @pl.when(i > 0)
            def _():
                second.ready(i)

        g = group_at(i)
        sums = []
        for q in range(blocks):
            cb = g * blocks + q
            s, j = cb // nb, lax.rem(cb, nb)
            cols = pl.ds(pl.multiple_of(cb * WIDE, WIDE), WIDE)
            base = pl.multiple_of(j * span, PACK)
            rows = lambda n: pl.ds(pl.multiple_of(base + rank + n * PACK, PACK), PACK)
            misc = w2[s, rows(2), :].astype(F32)
            rt[g, :, WIDE * q : WIDE * q + WIDE] = w2[s, rows(0), :].astype(F32) + w2[s, rows(1), :].astype(F32)
            raw = jnp.dot(nm[...], w2[s, pl.ds(base, rank), :], preferred_element_type=F32)
            raw = raw + (misc[0:1] + misc[2:3])
            small = jnp.exp2(jnp.abs(raw) * -LOG2E)
            step = jnp.maximum(raw, 0.0) + LN2 * jnp.log2(1.0 + small)
            st[:, :, cols] = step.reshape(tokens // ROWS8, ROWS8, WIDE)
            dr[:, :, cols] = (step * xv[:, cols].astype(F32)).reshape(tokens // ROWS8, ROWS8, WIDE)
            total = jnp.sum(step, axis=0, keepdims=True)
            sums += [total[:, :LANES], total[:, LANES:]]
        view = pl.ds(pl.multiple_of(g * GROUP, GROUP), GROUP)
        zero = jnp.zeros((ROWS8, LANES), F32)
        for part in range(0, tiles, TILES):
            h = scan_tokens(
                st.at[:, :, view], dr.at[:, :, view], bx, rt.at[g], (zero,) * (2 * TILES), tokens, strips(part)
            )
            for j in range(TILES):
                n = 16 * (part + j)
                eb[g, n : n + 16, :] = jnp.concatenate([h[j], h[TILES + j]], 0).astype(BF16)
        sums = jnp.concatenate(sums, 0)
        top = sums.astype(BF16).astype(F32)
        eb[g, 16 * tiles : 16 * tiles + 16, :] = jnp.concatenate([top, sums - top], 0).astype(BF16)

        @pl.when(g != me)
        def _():
            to_combiner(g).start()

        @pl.when(g == me)
        def _():
            rb[me] = eb[me]

        return 0

    if local_order:
        second.relay(1)
    else:
        def settle(i, _):
            second.relay(i)
            second.relay_plane(i)
            second.ready(i)
            return 0

        lax.fori_loop(1, D, settle, 0)
    with jax.named_scope("pass1"):
        lax.fori_loop(0, groups, pass_one, 0)

    def to_owner(k):
        return pltpu.make_async_remote_copy(
            src_ref=sb.at[k], dst_ref=h0b.at[me], send_sem=bs.at[k], recv_sem=br.at[me],
            device_id={"a": k // B, "b": lax.rem(k, B)}, device_id_type=MESH,
        )

    def arrival(k):
        return pltpu.make_async_remote_copy(
            src_ref=rb.at[k], dst_ref=rb.at[k], send_sem=es.at[0], recv_sem=er.at[k],
            device_id={"c": c}, device_id_type=MESH,
        )

    with jax.named_scope("combine"):
        @pl.when(me < groups)
        def _():
            def combine(k, start):
                @pl.when(k != me)
                def _():
                    arrival(k).wait_recv()

                now = []
                both = rb[k, 16 * tiles : 16 * tiles + 16, :].astype(F32)
                sums = both[0:8] + both[8:16]
                for j in range(tiles):
                    sb[k, 16 * j : 16 * j + 16, :] = start[j].astype(BF16)
                    decay = jnp.exp2(sums[j : j + 1, :] * rt[me, :, LANES * j : LANES * j + LANES])
                    now.append(decay * start[j] + rb[k, 16 * j : 16 * j + 16, :].astype(F32))

                @pl.when(k != me)
                def _():
                    to_owner(k).start()

                @pl.when(k == me)
                def _():
                    h0b[me] = sb[me]

                return tuple(now)

            lax.fori_loop(0, D, combine, (jnp.zeros((16, LANES), F32),) * tiles)

    loads[3].wait()

    def start_of(g):
        return pltpu.make_async_remote_copy(
            src_ref=h0b.at[g], dst_ref=h0b.at[g], send_sem=bs.at[0], recv_sem=br.at[g],
            device_id={"c": c}, device_id_type=MESH,
        )

    def put(g):
        view = pl.ds(pl.multiple_of(g * GROUP, GROUP), GROUP)
        return pltpu.make_async_copy(gv.at[:, view], out_hbm.at[:, view], osem.at[g])

    def pass_two(i, _):
        g = lax.rem(me + i, groups)

        @pl.when(g != me)
        def _():
            start_of(g).wait_recv()

        view = pl.ds(pl.multiple_of(g * GROUP, GROUP), GROUP)
        xg, gg = xv.at[:, view], gv.at[:, view]
        direct = []
        for q in range(blocks):
            cb = g * blocks + q
            s, j = cb // nb, lax.rem(cb, nb)
            misc = w2[s, pl.ds(pl.multiple_of(j * span + rank + 2 * PACK, PACK), PACK), :].astype(F32)
            both = misc[1:2] + misc[3:4]
            direct += [both[:, LANES * n : LANES * n + LANES] for n in range(WIDE // LANES)]
        for part in range(0, tiles, TILES):
            cols = strips(part)
            first_state = [h0b[g, 16 * j : 16 * j + 16, :].astype(F32) for j in range(part, part + TILES)]
            h = tuple(v[:8] for v in first_state) + tuple(v[8:] for v in first_state)

            def each(i, u, at, now):
                c0, c1 = (cx[pl.ds(at + 8 * k, 8), :] for k in range(2))
                for j in range(TILES):
                    n = PITCH * (STEP * j + u)
                    zb[n : n + 8, :] = c0 * now[0][j] + c1 * now[1][j]
                if u < STEP - 1:
                    return
                where = pl.ds(pl.multiple_of(i * STEP, STEP), STEP)
                for j in range(TILES):
                    halves = []
                    for t in range(0, STEP, 8):
                        o = [zb[pl.ds(PITCH * (STEP * j + t) + q, 8, stride=PITCH), :] for q in range(8)]
                        halves.append(((o[0] + o[1]) + (o[2] + o[3])) + ((o[4] + o[5]) + (o[6] + o[7])))
                    y = jnp.concatenate(halves, 0) + direct[part + j] * xg[where, cols[j]].astype(F32)
                    gg[where, cols[j]] = (y * silu(gg[where, cols[j]].astype(F32))).astype(BF16)

            scan_tokens(st.at[:, :, view], dr.at[:, :, view], bx, rt.at[g], h, tokens, cols, each)
        put(g).start()
        return 0

    with jax.named_scope("pass2"):
        lax.fori_loop(0, groups, pass_two, 0)

    def finish(g, _):
        put(g).wait()

        @pl.when(g != me)
        def _():
            to_combiner(g).wait_send()

        return 0

    with jax.named_scope("finish"):
        lax.fori_loop(0, groups, finish, 0)

        @pl.when(me < groups)
        def _():
            def sent(k, _):
                @pl.when(k != me)
                def _():
                    to_owner(k).wait_send()

                return 0

            lax.fori_loop(0, D, sent, 0)

        halo_copy.wait_send()
        first.drain()
        second.drain()


def local(sizes, conv_input, gate_input, conv_weight, conv_bias, x_weight, dt_gain, dt_weight, dt_bias, a_log, skip):
    A, B, X = sizes
    D = A * B
    tokens, inner = conv_input.shape
    rank, shard = dt_weight.shape
    states = a_log.shape[0]
    nb = shard // WIDE
    groups = inner // GROUP
    small = -(-(conv_weight.shape[0] + 1) * nb // PACK) * PACK
    r1 = padded_rows(x_weight.shape[1] * nb, X)
    r2 = padded_rows((rank + 3 * PACK) * nb, X)
    tiles = GROUP // LANES
    packet = 16 * tiles + 16
    hbm = pl.BlockSpec(memory_space=pl.ANY)
    vmem = pl.BlockSpec(memory_space=pltpu.VMEM)
    dma = pltpu.SemaphoreType.DMA
    return pl.pallas_call(
        functools.partial(mixer_kernel, sizes, states),
        in_specs=[hbm] * 4 + [vmem] * 6,
        out_specs=hbm,
        out_shape=jax.ShapeDtypeStruct((tokens, inner), BF16),
        scratch_shapes=[
            pltpu.VMEM((tokens, inner), BF16),
            pltpu.VMEM((tokens, inner), BF16),
            pltpu.VMEM((x_weight.shape[1], shard), BF16),
            pltpu.VMEM(dt_weight.shape, BF16),
            pltpu.VMEM((ROWS8, inner), BF16),
            pltpu.VMEM((D, small, WIDE), BF16),
            pltpu.VMEM((D, r1, WIDE), BF16),
            pltpu.VMEM((D, r2, WIDE), BF16),
            pltpu.VMEM((tokens, x_weight.shape[1]), F32),
            pltpu.VMEM((tokens, rank), BF16),
            pltpu.VMEM((tokens * states, LANES), F32),
            pltpu.VMEM((tokens * states, LANES), F32),
            pltpu.VMEM((tokens // ROWS8, ROWS8, inner), F32),
            pltpu.VMEM((tokens // ROWS8, ROWS8, inner), F32),
            pltpu.VMEM((groups, states, GROUP), F32),
            pltpu.VMEM((PITCH * STEP * TILES, LANES), F32),
            pltpu.VMEM((groups, packet, LANES), BF16),
            pltpu.VMEM((D, packet, LANES), BF16),
            pltpu.VMEM((D, 16 * tiles, LANES), BF16),
            pltpu.VMEM((groups, 16 * tiles, LANES), BF16),
            dma((4,)), dma((groups,)), dma((2,)), dma((2, A)), dma((B, A)), dma((D,)),
            dma((2, 2, A)), dma((2, B, A)), dma((2, X, D)), dma((2, X, D)),
            dma((2, D)), dma((2, X, D)), dma((2, X, D)),
            dma((groups,)), dma((D,)), dma((D,)), dma((groups,)),
        ],
        compiler_params=pltpu.CompilerParams(
            collective_id=0, has_side_effects=True, vmem_limit_bytes=60 * 1024 * 1024
        ),
        name="mixer",
    )(
        conv_input, gate_input, x_weight.T, dt_weight, conv_weight, conv_bias[None, :], dt_bias[None, :],
        skip[None, :], a_log, dt_gain[None, :],
    )


def solution(mesh):
    seq, batch = mesh.shape["seq"], mesh.shape["batch"]
    cores = 2
    A = math.gcd(seq, batch)
    B, X = seq // A, batch // cores
    grid = Mesh(mesh.devices.reshape(A, B, X, cores), ("a", "b", "x", "c"))
    seqs = ("a", "b")
    rows = P(("x", "c", "a", "b"), None)
    return jax.shard_map(
        functools.partial(local, (A, B, X)),
        mesh=grid,
        in_specs=(
            rows, rows, P(None, seqs), P(seqs), P(seqs, None), P(), P(None, seqs), P(seqs), P(None, seqs), P(seqs),
        ),
        out_specs=rows,
        check_vma=False,
    )
```

```python
import functools
import math

import jax
import jax.numpy as jnp
from jax import lax
from jax.experimental import pallas as pl
from jax.experimental.pallas import tpu as pltpu
from jax.sharding import Mesh
from jax.sharding import PartitionSpec as P

LOG2E = 1.4426950408889634
LN2 = 0.6931471805599453
LANES = 128
ROWS8 = 8
PACK = 16
WIDE = 256
GROUP = 1024
STEP = 16
TILES = 4
PITCH = 9
MESH = pl.DeviceIdType.MESH
F32 = jnp.float32
BF16 = jnp.bfloat16


def split_rows(rows, planes):
    half = rows // 2
    if planes == 2:
        private = -(-half // (3 * PACK)) * PACK
        return half, private, half - 2 * private
    return half, half // planes, 0


def padded_rows(rows, planes):
    unit = 2 * PACK * (planes if planes > 2 else 1)
    return -(-rows // unit) * unit


def column(a, i, size):
    turn = lax.rem(i, 2)
    inner = a + (1 - 2 * turn) * ((i + 1) // 2)
    outer = jnp.where(2 * a < size - 1, i, size - 1 - i)
    return jnp.where(i <= 2 * jnp.minimum(a, size - 1 - a), inner, outer)


def pieces_of(blocks):
    return 2 if blocks % 2 == 0 else 1


class Gather:
    def __init__(self, sizes, place, which, buf, base, rows, sems, small=None, small_sems=None):
        self.A, self.B, self.X = sizes
        self.a, self.b, self.x, self.c = place
        self.w = which
        self.buf = buf
        self.base = base
        (self.zs, self.ys, self.xs, self.ds, self.wr, self.xr, self.dr) = sems
        self.small = small
        self.small_sems = small_sems
        self.half, self.private, self.shared = split_rows(rows, self.X)

    def turn(self, t):
        block, r = (t - 1) // self.B, lax.rem(t - 1 + self.B, self.B)
        r = r + jnp.where(block == self.A - 1, 1, 0)
        near = jnp.where(r == 0, block + 1, r * self.A + block)
        return jnp.where(t == 0, 0, near)

    def shard(self, t):
        i = self.turn(t)
        a = column(self.a, lax.rem(i, self.A), self.A)
        return a * self.B + lax.rem(self.b - i // self.A + self.B, self.B)

    def window(self, s, core):
        start = self.base + core * self.half + self.x * self.private
        return self.buf.at[s, pl.ds(pl.multiple_of(start, PACK), self.private + self.shared)]

    def own(self, s, core, plane):
        start = self.base + core * self.half + plane * (self.private + self.shared)
        return self.buf.at[s, pl.ds(pl.multiple_of(start, PACK), self.private)]

    def copy(self, ref, send, recv, **to):
        return pltpu.make_async_remote_copy(
            src_ref=ref, dst_ref=ref, send_sem=send, recv_sem=recv,
            device_id=to, device_id_type=MESH,
        )

    def along(self, p, way):
        s = p * self.B + self.b
        to = self.a + 1 - 2 * way
        out = []
        if self.small is not None:
            zs, _, wr = self.small_sems
            out.append(self.copy(self.small.at[s], zs.at[way, p], wr.at[s], a=to))
        out.append(self.copy(self.window(s, self.c), self.zs.at[self.w, way, p], self.wr.at[self.w, s], a=to))
        return out

    def across(self, p, k):
        s = p * self.B + self.b
        to = lax.rem(self.b + k, self.B)
        out = []
        if self.small is not None:
            _, ys, wr = self.small_sems
            out.append(self.copy(self.small.at[s], ys.at[k, p], wr.at[s], b=to))
        out.append(self.copy(self.window(s, self.c), self.ys.at[self.w, k, p], self.wr.at[self.w, s], b=to))
        return out

    def plane(self, s, k):
        return self.copy(
            self.own(s, self.c, self.x), self.xs.at[self.w, k, s],
            self.xr.at[self.w, k, s], x=lax.rem(self.x + k, self.X),
        )

    def from_plane(self, s, k):
        ref = self.own(s, self.c, lax.rem(self.x - k + self.X, self.X))
        return self.copy(ref, self.xs.at[self.w, k, s], self.xr.at[self.w, k, s], x=self.x)

    def pair(self, s, e, core):
        if e == 0:
            ref = self.window(s, core)
        else:
            ref = self.own(s, core, lax.rem(self.x - e + self.X, self.X))
        return self.copy(ref, self.ds.at[self.w, e, s], self.dr.at[self.w, e, s], c=1 - self.c)

    def sends(self, p, right, left, run):
        @pl.when(right & (self.a + 1 < self.A))
        def _():
            run(self.along(p, 0))

        @pl.when(left & (self.a > 0))
        def _():
            run(self.along(p, 1))

    @staticmethod
    def start(copies):
        for copy in copies:
            copy.start()

    @staticmethod
    def sent(copies):
        for copy in copies:
            copy.wait_send()

    def begin_line(self):
        self.sends(self.a, self.a >= 0, self.a >= 0, self.start)

    def begin_side(self):
        for k in range(1, self.B):
            self.start(self.across(self.a, k))

    def relay(self, t):
        s = self.shard(t)
        p = s // self.B
        if self.small is not None:
            zs, _, wr = self.small_sems
            self.copy(self.small.at[s], zs.at[0, 0], wr.at[s], c=self.c).wait_recv()
        self.copy(self.window(s, self.c), self.zs.at[self.w, 0, 0], self.wr.at[self.w, s], c=self.c).wait_recv()

        @pl.when(lax.rem(s, self.B) == self.b)
        def _():
            self.sends(p, p < self.a, p > self.a, self.start)
            for k in range(1, self.B):
                self.start(self.across(p, k))

        for k in range(1, self.X):
            self.plane(s, k).start()
        self.pair(s, 0, self.c).start()

    def relay_plane(self, i):
        s = self.shard(i)
        for k in range(1, self.X):
            self.from_plane(s, k).wait_recv()
            self.pair(s, k, self.c).start()

    def ready(self, i):
        s = self.shard(i)
        for e in range(self.X):
            self.pair(s, e, 1 - self.c).wait_recv()

    def drain(self):
        def line(p, _):
            self.sends(p, p <= self.a, p >= self.a, self.sent)
            for k in range(1, self.B):
                self.sent(self.across(p, k))
            return 0

        lax.fori_loop(0, self.A, line, 0)

        def one(i, _):
            s = self.shard(i)
            for k in range(1, self.X):
                self.plane(s, k).wait_send()
            for e in range(self.X):
                self.pair(s, e, self.c).wait_send()
            return 0

        lax.fori_loop(1, self.A * self.B, one, 0)


def scan_tokens(st, dr, bx, rate, hidden, tokens, tiles, each=None):
    rates = [[rate[8 * k : 8 * k + 8, cols] for cols in tiles] for k in range(2)]
    count = len(tiles)

    def body(i, carry):
        h = [list(carry[:count]), list(carry[count:])]
        for u in range(STEP):
            at = pl.multiple_of((i * STEP + u) * 16, 16)
            b = [bx[pl.ds(at + 8 * k, 8), :] for k in range(2)]
            block = i * (STEP // ROWS8) + u // ROWS8
            row = slice(u % ROWS8, u % ROWS8 + 1)
            for j, cols in enumerate(tiles):
                s = jnp.broadcast_to(st[block, row, cols], (ROWS8, LANES))
                d = jnp.broadcast_to(dr[block, row, cols], (ROWS8, LANES))
                for k in range(2):
                    h[k][j] = jnp.exp2(s * rates[k][j]) * h[k][j] + b[k] * d
            if each is not None:
                each(i, u, at, h)
        return tuple(h[0]) + tuple(h[1])

    return lax.fori_loop(0, tokens // STEP, body, hidden)


def silu(v):
    half = 0.5 * v
    return half + half * jnp.tanh(half)


def mixer_kernel(
    sizes, states,
    x_hbm, g_hbm, xw_hbm, dtw_hbm, cw_ref, cb_ref, db_ref, sk_ref, al_ref, gain_ref,
    out_hbm,
    xv, gv, xwv, dtv, last, halo_out, halo, cp, w1, w2, acc, nm, bx, cx, st, dr, rt, zb,
    eb, rb, sb, h0b,
    lsem, osem, hsem, cz, cy, cr,
    zs, ys, xs, ds, wr, xr, dr_sem,
    es, er, bs, br,
):
    A, B, X = sizes
    D = A * B
    tokens, inner = xv.shape
    wide, shard = xwv.shape
    nb = shard // WIDE
    rank = gain_ref.shape[1]
    taps = cw_ref.shape[0]
    groups = inner // GROUP
    span = rank + 3 * PACK
    cuts = pieces_of(nb)
    part_blocks = nb // cuts
    rows1, rows2 = w1.shape[1] // cuts, w2.shape[1] // cuts
    spot1 = lambda j: (j // part_blocks) * rows1 + (j % part_blocks) * wide
    spot2 = lambda j: (j // part_blocks) * rows2 + (j % part_blocks) * span
    a, b, x, c = (lax.axis_index(n) for n in ("a", "b", "x", "c"))
    me = a * B + b
    place = (a, b, x, c)
    sems = (zs, ys, xs, ds, wr, xr, dr_sem)

    loads = [
        pltpu.make_async_copy(src, dst, lsem.at[n])
        for n, (src, dst) in enumerate(((xw_hbm, xwv), (dtw_hbm, dtv), (x_hbm, xv), (g_hbm, gv), (x_hbm.at[pl.ds(tokens - ROWS8, ROWS8)], last)))
    ]
    for n in (4, 0, 1, 2, 3):
        loads[n].start()

    barrier = pltpu.get_barrier_semaphore()
    for r in range(1, D):
        other = lax.rem(me + r, D)
        pl.semaphore_signal(
            barrier, inc=1, device_id={"a": other // B, "b": lax.rem(other, B)}, device_id_type=MESH
        )
    for k in range(1, X):
        pl.semaphore_signal(barrier, inc=1, device_id={"x": lax.rem(x + k, X)}, device_id_type=MESH)
    pl.semaphore_signal(barrier, inc=1, device_id={"c": 1 - c}, device_id_type=MESH)

    lanes = cb_ref[...].astype(F32)
    per = WIDE // LANES
    bias = lambda j: jnp.concatenate([lanes[n : n + 1] for n in range(per * j, per * j + per)], 1)
    weight = cw_ref[...].astype(F32)
    pieces = [r for j in range(nb) for r in (weight[:, WIDE * j : WIDE * j + WIDE], bias(j))]
    fill = cp.shape[1] - (taps + 1) * nb
    cp[me] = jnp.concatenate(pieces + [jnp.zeros((fill, WIDE), F32)], 0).astype(BF16)
    loads[4].wait()
    tail = last[...].astype(F32)
    fill = halo.shape[1] - (taps - 1) * nb
    for s in range(D):
        pieces = [
            tail[ROWS8 - taps + 1 :, n : n + WIDE] for n in range(s * shard, s * shard + shard, WIDE)
        ]
        halo_out[s] = jnp.concatenate(pieces + [jnp.zeros((fill, WIDE), F32)], 0).astype(BF16)
    loads[0].wait()
    for j in range(nb):
        w1[me, spot1(j) : spot1(j) + wide, :] = xwv[:, WIDE * j : WIDE * j + WIDE]
    with jax.named_scope("barrier"):
        pl.semaphore_wait(barrier, D - 1 + X - 1 + 1)

    after = lax.rem(me + 1, D)
    halo_copy = pltpu.make_async_remote_copy(
        src_ref=halo_out, dst_ref=halo, send_sem=hsem.at[0], recv_sem=hsem.at[1],
        device_id={"a": after // B, "b": lax.rem(after, B)}, device_id_type=MESH,
    )
    first = [
        Gather(sizes, place, n, w1, n * rows1, rows1, sems, *((cp, (cz, cy, cr)) if n == 0 else ()))
        for n in range(cuts)
    ]
    second = [Gather(sizes, place, cuts + n, w2, n * rows2, rows2, sems) for n in range(cuts)]
    halo_copy.start()
    for g in first:
        g.begin_line()
        g.begin_side()

    for j in range(nb):
        cols = slice(WIDE * j, WIDE * j + WIDE)
        rate = -jnp.exp(al_ref[:, cols]) * LOG2E
        high = rate.astype(BF16)
        base = spot2(j) + rank
        w2[me, base : base + states, :] = high
        w2[me, base + PACK : base + PACK + states, :] = (rate - high.astype(F32)).astype(BF16)
        two = jnp.concatenate([db_ref[:, cols], sk_ref[:, cols]], 0)
        top = two.astype(BF16).astype(F32)
        w2[me, base + 2 * PACK : base + 3 * PACK, :] = jnp.concatenate(
            [top, two - top, jnp.zeros((PACK - 4, WIDE), F32)], 0
        ).astype(BF16)
    loads[1].wait()
    for j in range(nb):
        w2[me, spot2(j) : spot2(j) + rank, :] = dtv[:, WIDE * j : WIDE * j + WIDE]
    loads[2].wait()
    acc[...] = jnp.zeros_like(acc)
    lead = (me > 0).astype(F32)
    shard_at = first[0].shard

    def convolve(i):
        s = shard_at(i)
        weight = cp[s].astype(F32)
        before = halo[s].astype(F32) * lead
        for j in range(nb):
            cols = pl.ds(pl.multiple_of(s * shard + WIDE * j, WIDE), WIDE)
            row = lambda n: weight[(taps + 1) * j + n : (taps + 1) * j + n + 1]
            cur = xv[:, cols].astype(F32)
            head = before[(taps - 1) * j : (taps - 1) * (j + 1)]
            ext = jnp.concatenate([jnp.zeros((ROWS8 - taps + 1, WIDE), F32), head, cur], 0)
            total = row(taps) + row(taps - 1) * cur
            for tap in range(taps - 1):
                low = ROWS8 - taps + 1 + tap
                total = total + row(tap) * ext[low : low + tokens]
            xv[:, cols] = silu(total).astype(BF16)

    def project(i):
        s = shard_at(i)
        if not isinstance(i, int) or i > 0:
            for g in first:
                g.ready(i)
        total = acc[...]
        for j in range(nb):
            cols = pl.ds(pl.multiple_of(s * shard + WIDE * j, WIDE), WIDE)
            total = total + lax.dot_general(
                xv[:, cols], w1[s, spot1(j) : spot1(j) + wide, :], (((1,), (1,)), ((), ())),
                preferred_element_type=F32,
            )
        acc[...] = total

    def step_first(t, _):
        for g in first:
            g.relay(t)

        @pl.when(t > 2)
        def _():
            for g in first:
                g.relay_plane(t - 2)

        @pl.when(t == 1)
        def _():
            halo_copy.wait_recv()

        convolve(t - 1)

        @pl.when(t > 4)
        def _():
            project(t - 4)

        return 0

    split = (A - 2) * B + 2
    with jax.named_scope("w1a"):
        lax.fori_loop(1, split, step_first, 0)
        for w in second:
            w.begin_line()
        lax.fori_loop(split, D, step_first, 0)
        for w in second:
            w.begin_side()
    with jax.named_scope("w1b"):
        convolve(D - 1)
        for g in first:
            g.relay_plane(D - 2)
        project(0)
        for w in second:
            w.relay(1)
        for g in first:
            g.relay_plane(D - 1)
        project(D - 4)
        project(D - 3)
        for w in second:
            w.relay(2)
        project(D - 2)
        project(D - 1)

    with jax.named_scope("norm"):
        low = acc[:, :rank]
        nm[...] = (
            low * lax.rsqrt(jnp.mean(low * low, axis=1, keepdims=True) + 1e-06) * gain_ref[...]
        ).astype(BF16)
        bc = acc[:, rank:]
        for n in range(states):
            at = pl.ds(n, tokens, stride=states)
            bx[at, :] = jnp.broadcast_to(bc[:, n : n + 1], (tokens, LANES))
            cx[at, :] = jnp.broadcast_to(bc[:, states + n : states + n + 1], (tokens, LANES))

    tiles = GROUP // LANES
    blocks = GROUP // WIDE
    local_order = groups == D

    def strips(part):
        return [slice(LANES * j, LANES * j + LANES) for j in range(part, part + TILES)]

    def group_at(i):
        return shard_at(i) if local_order else i

    def to_combiner(g):
        return pltpu.make_async_remote_copy(
            src_ref=eb.at[g], dst_ref=rb.at[me], send_sem=es.at[g], recv_sem=er.at[me],
            device_id={"a": g // B, "b": lax.rem(g, B)}, device_id_type=MESH,
        )

    def pass_one(i, _):
        if local_order:
            @pl.when(i + 3 < D)
            def _():
                for w in second:
                    w.relay(i + 3)

            @pl.when(i + 1 < D)
            def _():
                for w in second:
                    w.relay_plane(i + 1)

            @pl.when(i > 0)
            def _():
                for w in second:
                    w.ready(i)

        g = group_at(i)
        sums = []
        for q in range(blocks):
            cb = g * blocks + q
            s, j = cb // nb, lax.rem(cb, nb)
            cols = pl.ds(pl.multiple_of(cb * WIDE, WIDE), WIDE)
            base = pl.multiple_of(spot2(j), PACK)
            rows = lambda n: pl.ds(pl.multiple_of(base + rank + n * PACK, PACK), PACK)
            misc = w2[s, rows(2), :].astype(F32)
            rt[g, :, WIDE * q : WIDE * q + WIDE] = w2[s, rows(0), :].astype(F32) + w2[s, rows(1), :].astype(F32)
            raw = jnp.dot(nm[...], w2[s, pl.ds(base, rank), :], preferred_element_type=F32)
            raw = raw + (misc[0:1] + misc[2:3])
            small = jnp.exp2(jnp.abs(raw) * -LOG2E)
            step = jnp.maximum(raw, 0.0) + LN2 * jnp.log2(1.0 + small)
            st[:, :, cols] = step.reshape(tokens // ROWS8, ROWS8, WIDE)
            dr[:, :, cols] = (step * xv[:, cols].astype(F32)).reshape(tokens // ROWS8, ROWS8, WIDE)
            total = jnp.sum(step, axis=0, keepdims=True)
            sums += [total[:, :LANES], total[:, LANES:]]
        view = pl.ds(pl.multiple_of(g * GROUP, GROUP), GROUP)
        zero = jnp.zeros((ROWS8, LANES), F32)
        for part in range(0, tiles, TILES):
            h = scan_tokens(
                st.at[:, :, view], dr.at[:, :, view], bx, rt.at[g], (zero,) * (2 * TILES), tokens, strips(part)
            )
            for j in range(TILES):
                n = 16 * (part + j)
                eb[g, n : n + 16, :] = jnp.concatenate([h[j], h[TILES + j]], 0).astype(BF16)
        sums = jnp.concatenate(sums, 0)
        top = sums.astype(BF16).astype(F32)
        eb[g, 16 * tiles : 16 * tiles + 16, :] = jnp.concatenate([top, sums - top], 0).astype(BF16)

        @pl.when(g != me)
        def _():
            to_combiner(g).start()

        @pl.when(g == me)
        def _():
            rb[me] = eb[me]

        return 0

    def settle(i, _):
        for w in second:
            @pl.when(i > 2)
            def _():
                w.relay(i)

            w.relay_plane(i)
            w.ready(i)
        return 0

    if not local_order:
        lax.fori_loop(1, D, settle, 0)
    with jax.named_scope("pass1"):
        lax.fori_loop(0, groups, pass_one, 0)

    def to_owner(k):
        return pltpu.make_async_remote_copy(
            src_ref=sb.at[k], dst_ref=h0b.at[me], send_sem=bs.at[k], recv_sem=br.at[me],
            device_id={"a": k // B, "b": lax.rem(k, B)}, device_id_type=MESH,
        )

    def arrival(k):
        return pltpu.make_async_remote_copy(
            src_ref=rb.at[k], dst_ref=rb.at[k], send_sem=es.at[0], recv_sem=er.at[k],
            device_id={"c": c}, device_id_type=MESH,
        )

    with jax.named_scope("combine"):
        @pl.when(me < groups)
        def _():
            def combine(k, start):
                @pl.when(k != me)
                def _():
                    arrival(k).wait_recv()

                now = []
                both = rb[k, 16 * tiles : 16 * tiles + 16, :].astype(F32)
                sums = both[0:8] + both[8:16]
                for j in range(tiles):
                    sb[k, 16 * j : 16 * j + 16, :] = start[j].astype(BF16)
                    decay = jnp.exp2(sums[j : j + 1, :] * rt[me, :, LANES * j : LANES * j + LANES])
                    now.append(decay * start[j] + rb[k, 16 * j : 16 * j + 16, :].astype(F32))

                @pl.when(k != me)
                def _():
                    to_owner(k).start()

                @pl.when(k == me)
                def _():
                    h0b[me] = sb[me]

                return tuple(now)

            lax.fori_loop(0, D, combine, (jnp.zeros((16, LANES), F32),) * tiles)

    loads[3].wait()

    def start_of(g):
        return pltpu.make_async_remote_copy(
            src_ref=h0b.at[g], dst_ref=h0b.at[g], send_sem=bs.at[0], recv_sem=br.at[g],
            device_id={"c": c}, device_id_type=MESH,
        )

    def put(g):
        view = pl.ds(pl.multiple_of(g * GROUP, GROUP), GROUP)
        return pltpu.make_async_copy(gv.at[:, view], out_hbm.at[:, view], osem.at[g])

    def pass_two(i, _):
        g = lax.rem(me + i, groups)

        @pl.when(g != me)
        def _():
            start_of(g).wait_recv()

        view = pl.ds(pl.multiple_of(g * GROUP, GROUP), GROUP)
        xg, gg = xv.at[:, view], gv.at[:, view]
        direct = []
        for q in range(blocks):
            cb = g * blocks + q
            s, j = cb // nb, lax.rem(cb, nb)
            misc = w2[s, pl.ds(pl.multiple_of(spot2(j) + rank + 2 * PACK, PACK), PACK), :].astype(F32)
            both = misc[1:2] + misc[3:4]
            direct += [both[:, LANES * n : LANES * n + LANES] for n in range(WIDE // LANES)]
        for part in range(0, tiles, TILES):
            cols = strips(part)
            first_state = [h0b[g, 16 * j : 16 * j + 16, :].astype(F32) for j in range(part, part + TILES)]
            h = tuple(v[:8] for v in first_state) + tuple(v[8:] for v in first_state)

            def each(i, u, at, now):
                c0, c1 = (cx[pl.ds(at + 8 * k, 8), :] for k in range(2))
                for j in range(TILES):
                    n = PITCH * (STEP * j + u)
                    zb[n : n + 8, :] = c0 * now[0][j] + c1 * now[1][j]
                if u < STEP - 1:
                    return
                where = pl.ds(pl.multiple_of(i * STEP, STEP), STEP)
                for j in range(TILES):
                    halves = []
                    for t in range(0, STEP, 8):
                        o = [zb[pl.ds(PITCH * (STEP * j + t) + q, 8, stride=PITCH), :] for q in range(8)]
                        halves.append(((o[0] + o[1]) + (o[2] + o[3])) + ((o[4] + o[5]) + (o[6] + o[7])))
                    y = jnp.concatenate(halves, 0) + direct[part + j] * xg[where, cols[j]].astype(F32)
                    gg[where, cols[j]] = (y * silu(gg[where, cols[j]].astype(F32))).astype(BF16)

            scan_tokens(st.at[:, :, view], dr.at[:, :, view], bx, rt.at[g], h, tokens, cols, each)
        put(g).start()
        return 0

    with jax.named_scope("pass2"):
        lax.fori_loop(0, groups, pass_two, 0)

    def finish(g, _):
        put(g).wait()

        @pl.when(g != me)
        def _():
            to_combiner(g).wait_send()

        return 0

    with jax.named_scope("finish"):
        lax.fori_loop(0, groups, finish, 0)

        @pl.when(me < groups)
        def _():
            def sent(k, _):
                @pl.when(k != me)
                def _():
                    to_owner(k).wait_send()

                return 0

            lax.fori_loop(0, D, sent, 0)

        halo_copy.wait_send()
        for w in first + second:
            w.drain()


def local(sizes, conv_input, gate_input, conv_weight, conv_bias, x_weight, dt_gain, dt_weight, dt_bias, a_log, skip):
    A, B, X = sizes
    D = A * B
    tokens, inner = conv_input.shape
    rank, shard = dt_weight.shape
    states = a_log.shape[0]
    nb = shard // WIDE
    groups = inner // GROUP
    small = -(-(conv_weight.shape[0] + 1) * nb // PACK) * PACK
    edge = -(-(conv_weight.shape[0] - 1) * nb // PACK) * PACK
    cuts = pieces_of(nb)
    r1 = cuts * padded_rows(x_weight.shape[1] * nb // cuts, X)
    r2 = cuts * padded_rows((rank + 3 * PACK) * nb // cuts, X)
    tiles = GROUP // LANES
    packet = 16 * tiles + 16
    hbm = pl.BlockSpec(memory_space=pl.ANY)
    vmem = pl.BlockSpec(memory_space=pltpu.VMEM)
    dma = pltpu.SemaphoreType.DMA
    all_ = 2 * cuts
    return pl.pallas_call(
        functools.partial(mixer_kernel, sizes, states),
        in_specs=[hbm] * 4 + [vmem] * 6,
        out_specs=hbm,
        out_shape=jax.ShapeDtypeStruct((tokens, inner), BF16),
        scratch_shapes=[
            pltpu.VMEM((tokens, inner), BF16),
            pltpu.VMEM((tokens, inner), BF16),
            pltpu.VMEM((x_weight.shape[1], shard), BF16),
            pltpu.VMEM(dt_weight.shape, BF16),
            pltpu.VMEM((ROWS8, inner), BF16),
            pltpu.VMEM((D, edge, WIDE), BF16),
            pltpu.VMEM((D, edge, WIDE), BF16),
            pltpu.VMEM((D, small, WIDE), BF16),
            pltpu.VMEM((D, r1, WIDE), BF16),
            pltpu.VMEM((D, r2, WIDE), BF16),
            pltpu.VMEM((tokens, x_weight.shape[1]), F32),
            pltpu.VMEM((tokens, rank), BF16),
            pltpu.VMEM((tokens * states, LANES), F32),
            pltpu.VMEM((tokens * states, LANES), F32),
            pltpu.VMEM((tokens // ROWS8, ROWS8, inner), F32),
            pltpu.VMEM((tokens // ROWS8, ROWS8, inner), F32),
            pltpu.VMEM((groups, states, GROUP), F32),
            pltpu.VMEM((PITCH * STEP * TILES, LANES), F32),
            pltpu.VMEM((groups, packet, LANES), BF16),
            pltpu.VMEM((D, packet, LANES), BF16),
            pltpu.VMEM((D, 16 * tiles, LANES), BF16),
            pltpu.VMEM((groups, 16 * tiles, LANES), BF16),
            dma((5,)), dma((groups,)), dma((2,)), dma((2, A)), dma((B, A)), dma((D,)),
            dma((all_, 2, A)), dma((all_, B, A)), dma((all_, X, D)), dma((all_, X, D)),
            dma((all_, D)), dma((all_, X, D)), dma((all_, X, D)),
            dma((groups,)), dma((D,)), dma((D,)), dma((groups,)),
        ],
        compiler_params=pltpu.CompilerParams(
            collective_id=0, has_side_effects=True, vmem_limit_bytes=60 * 1024 * 1024
        ),
        name="mixer",
    )(
        conv_input, gate_input, x_weight.T, dt_weight, conv_weight, conv_bias.reshape(-1, LANES), dt_bias[None, :],
        skip[None, :], a_log, dt_gain[None, :],
    )


def solution(mesh):
    seq, batch = mesh.shape["seq"], mesh.shape["batch"]
    cores = 2
    A = math.gcd(seq, batch)
    B, X = seq // A, batch // cores
    grid = Mesh(mesh.devices.reshape(A, B, X, cores), ("a", "b", "x", "c"))
    seqs = ("a", "b")
    rows = P(("x", "c", "a", "b"), None)
    return jax.shard_map(
        functools.partial(local, (A, B, X)),
        mesh=grid,
        in_specs=(
            rows, rows, P(None, seqs), P(seqs), P(seqs, None), P(), P(None, seqs), P(seqs), P(None, seqs), P(seqs),
        ),
        out_specs=rows,
        check_vma=False,
    )
```

```python
import functools
import math

import jax
import jax.numpy as jnp
from jax import lax
from jax.experimental import pallas as pl
from jax.experimental.pallas import tpu as pltpu
from jax.sharding import Mesh
from jax.sharding import PartitionSpec as P

LOG2E = 1.4426950408889634
LN2 = 0.6931471805599453
LANES = 128
ROWS8 = 8
PACK = 16
WIDE = 256
GROUP = 1024
STEP = 32
TILES = 4
PITCH = 9
AHEAD = 9
CUTS = 2
SHARE = 0.34
MESH = pl.DeviceIdType.MESH
F32 = jnp.float32
BF16 = jnp.bfloat16


def split_rows(rows, planes):
    half = rows // 2
    if planes == 2:
        private = round(half * SHARE / PACK) * PACK
        return half, private, half - 2 * private
    return half, half // planes, 0


def padded_rows(rows, planes):
    unit = 2 * PACK * (planes if planes > 2 else 1)
    return -(-rows // unit) * unit


def column(a, i, size):
    turn = lax.rem(i, 2)
    inner = a + (1 - 2 * turn) * ((i + 1) // 2)
    outer = jnp.where(2 * a < size - 1, i, size - 1 - i)
    return jnp.where(i <= 2 * jnp.minimum(a, size - 1 - a), inner, outer)


def pieces_of(blocks):
    return math.gcd(blocks, CUTS)


class Gather:
    def __init__(self, sizes, place, which, buf, base, rows, sems, small=None, small_sems=None):
        self.A, self.B, self.X = sizes
        self.a, self.b, self.x, self.c = place
        self.w = which
        self.buf = buf
        self.base = base
        self.settled = False
        self.middle = (self.a > 0) & (self.a + 1 < self.A)
        (self.zs, self.ys, self.xs, self.ds, self.wr, self.xr, self.dr) = sems
        self.small = small
        self.small_sems = small_sems
        self.half, self.private, self.shared = split_rows(rows, self.X)

    def turn(self, t):
        block, r = (t - 1) // self.B, lax.rem(t - 1 + self.B, self.B)
        r = r + jnp.where(block == self.A - 1, 1, 0)
        near = jnp.where(r == 0, block + 1, r * self.A + block)
        if self.B == 2 and self.A > 2:
            near = jnp.where(self.middle & (t == 2), 2, jnp.where(self.middle & (t == 3), self.A, near))
            near = jnp.where(self.middle & (t == 4), 3, jnp.where(self.middle & (t == 5), self.A + 1, near))
        return jnp.where(t == 0, 0, near)

    def shard(self, t):
        i = self.turn(t)
        a = column(self.a, lax.rem(i, self.A), self.A)
        return a * self.B + lax.rem(self.b - i // self.A + self.B, self.B)

    def window(self, s, core):
        start = self.base + core * self.half + self.x * self.private
        return self.buf.at[s, pl.ds(pl.multiple_of(start, PACK), self.private + self.shared)]

    def own(self, s, core, plane):
        start = self.base + core * self.half + plane * (self.private + self.shared)
        return self.buf.at[s, pl.ds(pl.multiple_of(start, PACK), self.private)]

    def copy(self, ref, send, recv, **to):
        return pltpu.make_async_remote_copy(
            src_ref=ref, dst_ref=ref, send_sem=send, recv_sem=recv,
            device_id=to, device_id_type=MESH,
        )

    def along(self, p, way):
        s = p * self.B + self.b
        to = self.a + 1 - 2 * way
        out = []
        if self.small is not None:
            zs, _, wr = self.small_sems
            out.append(self.copy(self.small.at[s], zs.at[way, p], wr.at[s], a=to))
        out.append(self.copy(self.window(s, self.c), self.zs.at[self.w, way, p], self.wr.at[self.w, s], a=to))
        return out

    def across(self, p, k):
        s = p * self.B + self.b
        to = lax.rem(self.b + k, self.B)
        out = []
        if self.small is not None:
            _, ys, wr = self.small_sems
            out.append(self.copy(self.small.at[s], ys.at[k, p], wr.at[s], b=to))
        out.append(self.copy(self.window(s, self.c), self.ys.at[self.w, k, p], self.wr.at[self.w, s], b=to))
        return out

    def plane(self, s, k):
        return self.copy(
            self.own(s, self.c, self.x), self.xs.at[self.w, k, s],
            self.xr.at[self.w, k, s], x=lax.rem(self.x + k, self.X),
        )

    def from_plane(self, s, k):
        ref = self.own(s, self.c, lax.rem(self.x - k + self.X, self.X))
        return self.copy(ref, self.xs.at[self.w, k, s], self.xr.at[self.w, k, s], x=self.x)

    def pair(self, s, e, core):
        if e == 0:
            ref = self.window(s, core)
        else:
            ref = self.own(s, core, lax.rem(self.x - e + self.X, self.X))
        return self.copy(ref, self.ds.at[self.w, e, s], self.dr.at[self.w, e, s], c=1 - self.c)

    def sends(self, p, right, left, run):
        @pl.when(right & (self.a + 1 < self.A))
        def _():
            run(self.along(p, 0))

        @pl.when(left & (self.a > 0))
        def _():
            run(self.along(p, 1))

    @staticmethod
    def start(copies):
        for copy in copies:
            copy.start()

    @staticmethod
    def sent(copies):
        for copy in copies:
            copy.wait_send()

    def begin_line(self):
        self.sends(self.a, self.a >= 0, self.a >= 0, self.start)

    def begin_side(self):
        for k in range(1, self.B):
            self.start(self.across(self.a, k))

    def own_sent(self):
        self.settled = True
        self.sends(self.a, self.a >= 0, self.a >= 0, self.sent)
        for k in range(1, self.B):
            self.sent(self.across(self.a, k))

    def relay(self, t):
        s = self.shard(t)
        p = s // self.B
        if self.small is not None:
            zs, _, wr = self.small_sems
            self.copy(self.small.at[s], zs.at[0, 0], wr.at[s], c=self.c).wait_recv()
        self.copy(self.window(s, self.c), self.zs.at[self.w, 0, 0], self.wr.at[self.w, s], c=self.c).wait_recv()

        @pl.when(lax.rem(s, self.B) == self.b)
        def _():
            self.sends(p, p < self.a, p > self.a, self.start)
            for k in range(1, self.B):
                self.start(self.across(p, k))

        for k in range(1, self.X):
            self.plane(s, k).start()
        self.pair(s, 0, self.c).start()

    def relay_plane(self, i):
        s = self.shard(i)
        for k in range(1, self.X):
            self.from_plane(s, k).wait_recv()
            self.pair(s, k, self.c).start()

    def ready(self, i):
        s = self.shard(i)
        for e in range(self.X):
            self.pair(s, e, 1 - self.c).wait_recv()

    def drain(self):
        def line(p, _):
            @pl.when((p != self.a) | (not self.settled))
            def _():
                self.sends(p, p <= self.a, p >= self.a, self.sent)
                for k in range(1, self.B):
                    self.sent(self.across(p, k))

            return 0

        lax.fori_loop(0, self.A, line, 0)

        def one(i, _):
            s = self.shard(i)
            for k in range(1, self.X):
                self.plane(s, k).wait_send()
            for e in range(self.X):
                self.pair(s, e, self.c).wait_send()
            return 0

        lax.fori_loop(1, self.A * self.B, one, 0)


def scan_tokens(st, dr, bx, rate, hidden, tokens, tiles, each=None):
    rates = [[rate[8 * k : 8 * k + 8, cols] for cols in tiles] for k in range(2)]
    count = len(tiles)

    def body(i, carry):
        h = [list(carry[:count]), list(carry[count:])]
        for u in range(STEP):
            at = pl.multiple_of((i * STEP + u) * 16, 16)
            b = [bx[pl.ds(at + 8 * k, 8), :] for k in range(2)]
            block = i * (STEP // ROWS8) + u // ROWS8
            row = slice(u % ROWS8, u % ROWS8 + 1)
            for j, cols in enumerate(tiles):
                s = jnp.broadcast_to(st[block, row, cols], (ROWS8, LANES))
                d = jnp.broadcast_to(dr[block, row, cols], (ROWS8, LANES))
                for k in range(2):
                    h[k][j] = jnp.exp2(s * rates[k][j]) * h[k][j] + b[k] * d
            if each is not None:
                each(i, u, at, h)
        return tuple(h[0]) + tuple(h[1])

    return lax.fori_loop(0, tokens // STEP, body, hidden)


def silu(v):
    half = 0.5 * v
    return half + half * jnp.tanh(half)


def mixer_kernel(
    sizes, states,
    x_hbm, g_hbm, xw_hbm, dtw_hbm, cw_ref, cb_ref, db_ref, sk_ref, al_ref, gain_ref,
    out_hbm,
    xv, gv, xwv, dtv, last, halo_out, halo, cp, w1, w2, acc, nm, bx, cx, st, dr, rt, zb,
    eb, rb, sb, h0b,
    lsem, osem, hsem, cz, cy, cr,
    zs, ys, xs, ds, wr, xr, dr_sem,
    es, er, bs, br,
):
    A, B, X = sizes
    D = A * B
    tokens, inner = xv.shape
    wide, shard = xwv.shape
    nb = shard // WIDE
    rank = gain_ref.shape[1]
    taps = cw_ref.shape[0]
    groups = inner // GROUP
    span = rank + 3 * PACK
    cuts = pieces_of(nb)
    part_blocks = nb // cuts
    rows1, rows2 = w1.shape[1] // cuts, w2.shape[1] // cuts
    spot1 = lambda j: (j // part_blocks) * rows1 + (j % part_blocks) * wide
    spot2 = lambda j: (j // part_blocks) * rows2 + (j % part_blocks) * span
    a, b, x, c = (lax.axis_index(n) for n in ("a", "b", "x", "c"))
    me = a * B + b
    place = (a, b, x, c)
    sems = (zs, ys, xs, ds, wr, xr, dr_sem)

    loads = [
        pltpu.make_async_copy(src, dst, lsem.at[n])
        for n, (src, dst) in enumerate(((xw_hbm, xwv), (dtw_hbm, dtv), (x_hbm, xv), (g_hbm, gv), (x_hbm.at[pl.ds(tokens - ROWS8, ROWS8)], last)))
    ]
    for n in (4, 0, 1, 2, 3):
        loads[n].start()

    barrier = pltpu.get_barrier_semaphore()
    for r in range(1, D):
        other = lax.rem(me + r, D)
        pl.semaphore_signal(
            barrier, inc=1, device_id={"a": other // B, "b": lax.rem(other, B)}, device_id_type=MESH
        )
    for k in range(1, X):
        pl.semaphore_signal(barrier, inc=1, device_id={"x": lax.rem(x + k, X)}, device_id_type=MESH)
    pl.semaphore_signal(barrier, inc=1, device_id={"c": 1 - c}, device_id_type=MESH)

    lanes = cb_ref[...].astype(F32)
    per = WIDE // LANES
    bias = lambda j: jnp.concatenate([lanes[n : n + 1] for n in range(per * j, per * j + per)], 1)
    weight = cw_ref[...].astype(F32)
    pieces = [r for j in range(nb) for r in (weight[:, WIDE * j : WIDE * j + WIDE], bias(j))]
    fill = cp.shape[1] - (taps + 1) * nb
    cp[me] = jnp.concatenate(pieces + [jnp.zeros((fill, WIDE), F32)], 0).astype(BF16)
    loads[4].wait()
    tail = last[...].astype(F32)
    fill = halo.shape[1] - (taps - 1) * nb
    for s in range(D):
        pieces = [
            tail[ROWS8 - taps + 1 :, n : n + WIDE] for n in range(s * shard, s * shard + shard, WIDE)
        ]
        halo_out[s] = jnp.concatenate(pieces + [jnp.zeros((fill, WIDE), F32)], 0).astype(BF16)
    loads[0].wait()
    for j in range(nb):
        w1[me, spot1(j) : spot1(j) + wide, :] = xwv[:, WIDE * j : WIDE * j + WIDE]
    with jax.named_scope("barrier"):
        pl.semaphore_wait(barrier, D - 1 + X - 1 + 1)

    after = lax.rem(me + 1, D)
    halo_copy = pltpu.make_async_remote_copy(
        src_ref=halo_out, dst_ref=halo, send_sem=hsem.at[0], recv_sem=hsem.at[1],
        device_id={"a": after // B, "b": lax.rem(after, B)}, device_id_type=MESH,
    )
    first = [
        Gather(sizes, place, n, w1, n * rows1, rows1, sems, *((cp, (cz, cy, cr)) if n == 0 else ()))
        for n in range(cuts)
    ]
    second = [Gather(sizes, place, cuts + n, w2, n * rows2, rows2, sems) for n in range(cuts)]
    halo_copy.start()
    for n, g in enumerate(first):
        if n >= AHEAD:
            first[n - AHEAD].own_sent()
        g.begin_line()
        g.begin_side()

    for j in range(nb):
        cols = slice(WIDE * j, WIDE * j + WIDE)
        rate = -jnp.exp(al_ref[:, cols]) * LOG2E
        high = rate.astype(BF16)
        base = spot2(j) + rank
        w2[me, base : base + states, :] = high
        w2[me, base + PACK : base + PACK + states, :] = (rate - high.astype(F32)).astype(BF16)
        two = jnp.concatenate([db_ref[:, cols], sk_ref[:, cols]], 0)
        top = two.astype(BF16).astype(F32)
        w2[me, base + 2 * PACK : base + 3 * PACK, :] = jnp.concatenate(
            [top, two - top, jnp.zeros((PACK - 4, WIDE), F32)], 0
        ).astype(BF16)
    loads[1].wait()
    for j in range(nb):
        w2[me, spot2(j) : spot2(j) + rank, :] = dtv[:, WIDE * j : WIDE * j + WIDE]
    loads[2].wait()
    acc[...] = jnp.zeros_like(acc)
    lead = (me > 0).astype(F32)
    shard_at = first[0].shard

    def convolve(i):
        s = shard_at(i)
        weight = cp[s].astype(F32)
        before = halo[s].astype(F32) * lead
        for j in range(nb):
            cols = pl.ds(pl.multiple_of(s * shard + WIDE * j, WIDE), WIDE)
            row = lambda n: weight[(taps + 1) * j + n : (taps + 1) * j + n + 1]
            cur = xv[:, cols].astype(F32)
            head = before[(taps - 1) * j : (taps - 1) * (j + 1)]
            ext = jnp.concatenate([jnp.zeros((ROWS8 - taps + 1, WIDE), F32), head, cur], 0)
            total = row(taps) + row(taps - 1) * cur
            for tap in range(taps - 1):
                low = ROWS8 - taps + 1 + tap
                total = total + row(tap) * ext[low : low + tokens]
            xv[:, cols] = silu(total).astype(BF16)

    def project(i):
        s = shard_at(i)
        if not isinstance(i, int) or i > 0:
            for g in first:
                g.ready(i)
        total = acc[...]
        for j in range(nb):
            cols = pl.ds(pl.multiple_of(s * shard + WIDE * j, WIDE), WIDE)
            total = total + lax.dot_general(
                xv[:, cols], w1[s, spot1(j) : spot1(j) + wide, :], (((1,), (1,)), ((), ())),
                preferred_element_type=F32,
            )
        acc[...] = total

    def step_first(t, _):
        for g in first:
            g.relay(t)

        @pl.when(t > 3)
        def _():
            for g in first:
                g.relay_plane(t - 3)

        @pl.when(t == 1)
        def _():
            halo_copy.wait_recv()

        convolve(t - 1)

        @pl.when(t > 5)
        def _():
            project(t - 5)

        return 0

    split = (A - 2) * B + 2
    with jax.named_scope("w1a"):
        lax.fori_loop(1, split, step_first, 0)
        for w in second:
            w.begin_line()
        lax.fori_loop(split, D, step_first, 0)
        for w in second:
            w.begin_side()
    middle = second[0].middle

    def second_relay(t, when):
        @pl.when(when)
        def _():
            for w in second:
                w.relay(t)

    with jax.named_scope("w1b"):
        convolve(D - 1)
        for t in (D - 3, D - 2):
            for g in first:
                g.relay_plane(t)
        project(0)
        for w in second:
            w.relay(1)
        second_relay(2, middle)
        for g in first:
            g.relay_plane(D - 1)
        for t in range(D - 5, D):
            project(t)

    with jax.named_scope("norm"):
        low = acc[:, :rank]
        nm[...] = (
            low * lax.rsqrt(jnp.mean(low * low, axis=1, keepdims=True) + 1e-06) * gain_ref[...]
        ).astype(BF16)
        bc = acc[:, rank:]
        for n in range(states):
            at = pl.ds(n, tokens, stride=states)
            bx[at, :] = jnp.broadcast_to(bc[:, n : n + 1], (tokens, LANES))
            cx[at, :] = jnp.broadcast_to(bc[:, states + n : states + n + 1], (tokens, LANES))
        second_relay(2, jnp.logical_not(middle))
        for w in second:
            w.relay_plane(1)

    tiles = GROUP // LANES
    blocks = GROUP // WIDE
    local_order = groups == D

    def strips(part):
        return [slice(LANES * j, LANES * j + LANES) for j in range(part, part + TILES)]

    def group_at(i):
        return shard_at(i) if local_order else i

    def to_combiner(g):
        return pltpu.make_async_remote_copy(
            src_ref=eb.at[g], dst_ref=rb.at[me], send_sem=es.at[g], recv_sem=er.at[me],
            device_id={"a": g // B, "b": lax.rem(g, B)}, device_id_type=MESH,
        )

    def pass_one(i, _):
        if local_order:
            @pl.when(i + 3 < D)
            def _():
                for w in second:
                    w.relay(i + 3)

            @pl.when(i > 0)
            def _():
                for w in second:
                    w.ready(i)

        g = group_at(i)
        sums = []
        for q in range(blocks):
            cb = g * blocks + q
            s, j = cb // nb, lax.rem(cb, nb)
            cols = pl.ds(pl.multiple_of(cb * WIDE, WIDE), WIDE)
            base = pl.multiple_of(spot2(j), PACK)
            rows = lambda n: pl.ds(pl.multiple_of(base + rank + n * PACK, PACK), PACK)
            misc = w2[s, rows(2), :].astype(F32)
            rt[g, :, WIDE * q : WIDE * q + WIDE] = w2[s, rows(0), :].astype(F32) + w2[s, rows(1), :].astype(F32)
            raw = jnp.dot(nm[...], w2[s, pl.ds(base, rank), :], preferred_element_type=F32)
            raw = raw + (misc[0:1] + misc[2:3])
            small = jnp.exp2(jnp.abs(raw) * -LOG2E)
            step = jnp.maximum(raw, 0.0) + LN2 * jnp.log2(1.0 + small)
            st[:, :, cols] = step.reshape(tokens // ROWS8, ROWS8, WIDE)
            dr[:, :, cols] = (step * xv[:, cols].astype(F32)).reshape(tokens // ROWS8, ROWS8, WIDE)
            total = jnp.sum(step, axis=0, keepdims=True)
            sums += [total[:, :LANES], total[:, LANES:]]
        view = pl.ds(pl.multiple_of(g * GROUP, GROUP), GROUP)
        zero = jnp.zeros((ROWS8, LANES), F32)
        for part in range(0, tiles, TILES):
            h = scan_tokens(
                st.at[:, :, view], dr.at[:, :, view], bx, rt.at[g], (zero,) * (2 * TILES), tokens, strips(part)
            )
            if local_order and part == 0:
                @pl.when(i + 2 < D)
                def _():
                    with jax.named_scope("pl"):
                        for w in second:
                            w.relay_plane(i + 2)

            for j in range(TILES):
                n = 16 * (part + j)
                eb[g, n : n + 16, :] = jnp.concatenate([h[j], h[TILES + j]], 0).astype(BF16)
        sums = jnp.concatenate(sums, 0)
        top = sums.astype(BF16).astype(F32)
        eb[g, 16 * tiles : 16 * tiles + 16, :] = jnp.concatenate([top, sums - top], 0).astype(BF16)

        @pl.when(g != me)
        def _():
            to_combiner(g).start()

        @pl.when(g == me)
        def _():
            rb[me] = eb[me]

        return 0

    def settle(i, _):
        for w in second:
            @pl.when(i > 2)
            def _():
                w.relay(i)

            @pl.when(i > 1)
            def _():
                w.relay_plane(i)

            w.ready(i)
        return 0

    if not local_order:
        lax.fori_loop(1, D, settle, 0)
    with jax.named_scope("pass1"):
        lax.fori_loop(0, groups, pass_one, 0)

    def to_owner(k):
        return pltpu.make_async_remote_copy(
            src_ref=sb.at[k], dst_ref=h0b.at[me], send_sem=bs.at[k], recv_sem=br.at[me],
            device_id={"a": k // B, "b": lax.rem(k, B)}, device_id_type=MESH,
        )

    def arrival(k):
        return pltpu.make_async_remote_copy(
            src_ref=rb.at[k], dst_ref=rb.at[k], send_sem=es.at[0], recv_sem=er.at[k],
            device_id={"c": c}, device_id_type=MESH,
        )

    with jax.named_scope("combine"):
        @pl.when(me < groups)
        def _():
            def combine(k, start):
                @pl.when(k != me)
                def _():
                    arrival(k).wait_recv()

                now = []
                both = rb[k, 16 * tiles : 16 * tiles + 16, :].astype(F32)
                sums = both[0:8] + both[8:16]
                for j in range(tiles):
                    sb[k, 16 * j : 16 * j + 16, :] = start[j].astype(BF16)
                    decay = jnp.exp2(sums[j : j + 1, :] * rt[me, :, LANES * j : LANES * j + LANES])
                    now.append(decay * start[j] + rb[k, 16 * j : 16 * j + 16, :].astype(F32))

                @pl.when(k != me)
                def _():
                    to_owner(k).start()

                @pl.when(k == me)
                def _():
                    h0b[me] = sb[me]

                return tuple(now)

            lax.fori_loop(0, D, combine, (jnp.zeros((16, LANES), F32),) * tiles)

    loads[3].wait()

    def start_of(g):
        return pltpu.make_async_remote_copy(
            src_ref=h0b.at[g], dst_ref=h0b.at[g], send_sem=bs.at[0], recv_sem=br.at[g],
            device_id={"c": c}, device_id_type=MESH,
        )

    def put(g):
        view = pl.ds(pl.multiple_of(g * GROUP, GROUP), GROUP)
        return pltpu.make_async_copy(gv.at[:, view], out_hbm.at[:, view], osem.at[g])

    def pass_two(i, _):
        g = lax.rem(me + i, groups)

        @pl.when(g != me)
        def _():
            start_of(g).wait_recv()

        view = pl.ds(pl.multiple_of(g * GROUP, GROUP), GROUP)
        xg, gg = xv.at[:, view], gv.at[:, view]
        direct = []
        for q in range(blocks):
            cb = g * blocks + q
            s, j = cb // nb, lax.rem(cb, nb)
            misc = w2[s, pl.ds(pl.multiple_of(spot2(j) + rank + 2 * PACK, PACK), PACK), :].astype(F32)
            both = misc[1:2] + misc[3:4]
            direct += [both[:, LANES * n : LANES * n + LANES] for n in range(WIDE // LANES)]
        for part in range(0, tiles, TILES):
            cols = strips(part)
            first_state = [h0b[g, 16 * j : 16 * j + 16, :].astype(F32) for j in range(part, part + TILES)]
            h = tuple(v[:8] for v in first_state) + tuple(v[8:] for v in first_state)

            def each(i, u, at, now):
                c0, c1 = (cx[pl.ds(at + 8 * k, 8), :] for k in range(2))
                for j in range(TILES):
                    n = PITCH * (STEP * j + u)
                    zb[n : n + 8, :] = c0 * now[0][j] + c1 * now[1][j]
                if u < STEP - 1:
                    return
                where = pl.ds(pl.multiple_of(i * STEP, STEP), STEP)
                for j in range(TILES):
                    halves = []
                    for t in range(0, STEP, 8):
                        o = [zb[pl.ds(PITCH * (STEP * j + t) + q, 8, stride=PITCH), :] for q in range(8)]
                        halves.append(((o[0] + o[1]) + (o[2] + o[3])) + ((o[4] + o[5]) + (o[6] + o[7])))
                    y = jnp.concatenate(halves, 0) + direct[part + j] * xg[where, cols[j]].astype(F32)
                    gg[where, cols[j]] = (y * silu(gg[where, cols[j]].astype(F32))).astype(BF16)

            scan_tokens(st.at[:, :, view], dr.at[:, :, view], bx, rt.at[g], h, tokens, cols, each)
        put(g).start()
        return 0

    with jax.named_scope("pass2"):
        lax.fori_loop(0, groups, pass_two, 0)

    def finish(g, _):
        put(g).wait()

        @pl.when(g != me)
        def _():
            to_combiner(g).wait_send()

        return 0

    with jax.named_scope("finish"):
        lax.fori_loop(0, groups, finish, 0)

        @pl.when(me < groups)
        def _():
            def sent(k, _):
                @pl.when(k != me)
                def _():
                    to_owner(k).wait_send()

                return 0

            lax.fori_loop(0, D, sent, 0)

        halo_copy.wait_send()
        for w in first + second:
            w.drain()


def local(sizes, conv_input, gate_input, conv_weight, conv_bias, x_weight, dt_gain, dt_weight, dt_bias, a_log, skip):
    A, B, X = sizes
    D = A * B
    tokens, inner = conv_input.shape
    rank, shard = dt_weight.shape
    states = a_log.shape[0]
    nb = shard // WIDE
    groups = inner // GROUP
    small = -(-(conv_weight.shape[0] + 1) * nb // PACK) * PACK
    edge = -(-(conv_weight.shape[0] - 1) * nb // PACK) * PACK
    cuts = pieces_of(nb)
    r1 = cuts * padded_rows(x_weight.shape[1] * nb // cuts, X)
    r2 = cuts * padded_rows((rank + 3 * PACK) * nb // cuts, X)
    tiles = GROUP // LANES
    packet = 16 * tiles + 16
    hbm = pl.BlockSpec(memory_space=pl.ANY)
    vmem = pl.BlockSpec(memory_space=pltpu.VMEM)
    dma = pltpu.SemaphoreType.DMA
    all_ = 2 * cuts
    return pl.pallas_call(
        functools.partial(mixer_kernel, sizes, states),
        in_specs=[hbm] * 4 + [vmem] * 6,
        out_specs=hbm,
        out_shape=jax.ShapeDtypeStruct((tokens, inner), BF16),
        scratch_shapes=[
            pltpu.VMEM((tokens, inner), BF16),
            pltpu.VMEM((tokens, inner), BF16),
            pltpu.VMEM((x_weight.shape[1], shard), BF16),
            pltpu.VMEM(dt_weight.shape, BF16),
            pltpu.VMEM((ROWS8, inner), BF16),
            pltpu.VMEM((D, edge, WIDE), BF16),
            pltpu.VMEM((D, edge, WIDE), BF16),
            pltpu.VMEM((D, small, WIDE), BF16),
            pltpu.VMEM((D, r1, WIDE), BF16),
            pltpu.VMEM((D, r2, WIDE), BF16),
            pltpu.VMEM((tokens, x_weight.shape[1]), F32),
            pltpu.VMEM((tokens, rank), BF16),
            pltpu.VMEM((tokens * states, LANES), F32),
            pltpu.VMEM((tokens * states, LANES), F32),
            pltpu.VMEM((tokens // ROWS8, ROWS8, inner), F32),
            pltpu.VMEM((tokens // ROWS8, ROWS8, inner), F32),
            pltpu.VMEM((groups, states, GROUP), F32),
            pltpu.VMEM((PITCH * STEP * TILES, LANES), F32),
            pltpu.VMEM((groups, packet, LANES), BF16),
            pltpu.VMEM((D, packet, LANES), BF16),
            pltpu.VMEM((D, 16 * tiles, LANES), BF16),
            pltpu.VMEM((groups, 16 * tiles, LANES), BF16),
            dma((5,)), dma((groups,)), dma((2,)), dma((2, A)), dma((B, A)), dma((D,)),
            dma((all_, 2, A)), dma((all_, B, A)), dma((all_, X, D)), dma((all_, X, D)),
            dma((all_, D)), dma((all_, X, D)), dma((all_, X, D)),
            dma((groups,)), dma((D,)), dma((D,)), dma((groups,)),
        ],
        compiler_params=pltpu.CompilerParams(
            collective_id=0, has_side_effects=True, vmem_limit_bytes=60 * 1024 * 1024
        ),
        name="mixer",
    )(
        conv_input, gate_input, x_weight.T, dt_weight, conv_weight, conv_bias.reshape(-1, LANES), dt_bias[None, :],
        skip[None, :], a_log, dt_gain[None, :],
    )


def solution(mesh):
    seq, batch = mesh.shape["seq"], mesh.shape["batch"]
    cores = 2
    A = math.gcd(seq, batch)
    B, X = seq // A, batch // cores
    grid = Mesh(mesh.devices.reshape(A, B, X, cores), ("a", "b", "x", "c"))
    seqs = ("a", "b")
    rows = P(("x", "c", "a", "b"), None)
    return jax.shard_map(
        functools.partial(local, (A, B, X)),
        mesh=grid,
        in_specs=(
            rows, rows, P(None, seqs), P(seqs), P(seqs, None), P(), P(None, seqs), P(seqs), P(None, seqs), P(seqs),
        ),
        out_specs=rows,
        check_vma=False,
    )
```

```python
import functools
import math

import jax
import jax.numpy as jnp
from jax import lax
from jax.experimental import pallas as pl
from jax.experimental.pallas import tpu as pltpu
from jax.sharding import Mesh
from jax.sharding import PartitionSpec as P

LOG2E = 1.4426950408889634
LN2 = 0.6931471805599453
LANES = 128
ROWS8 = 8
PACK = 16
WIDE = 256
GROUP = 1024
STEP = 32
TILES = 4
PITCH = 9
AHEAD = 9
CUTS = 2
SHARE = 0.34
PARTS = 4
VMEM_MAIN = 48 * 1024 * 1024
VMEM_COPY = 4 * 1024 * 1024
MESH = pl.DeviceIdType.MESH
F32 = jnp.float32
BF16 = jnp.bfloat16


def split_rows(rows, planes):
    half = rows // 2
    if planes == 2:
        private = round(half * SHARE / PACK) * PACK
        return half, private, half - 2 * private
    return half, half // planes, 0


def padded_rows(rows, planes):
    unit = 2 * PACK * (planes if planes > 2 else 1)
    return -(-rows // unit) * unit


def column(a, i, size):
    turn = lax.rem(i, 2)
    inner = a + (1 - 2 * turn) * ((i + 1) // 2)
    outer = jnp.where(2 * a < size - 1, i, size - 1 - i)
    return jnp.where(i <= 2 * jnp.minimum(a, size - 1 - a), inner, outer)


def pieces_of(blocks):
    return math.gcd(blocks, CUTS)


class Gather:
    def __init__(self, sizes, place, which, buf, base, rows, sems, small=None, small_sems=None):
        self.A, self.B, self.X = sizes
        self.a, self.b, self.x, self.c = place
        self.w = which
        self.buf = buf
        self.base = base
        self.settled = False
        self.middle = (self.a > 0) & (self.a + 1 < self.A)
        (self.zs, self.ys, self.xs, self.ds, self.wr, self.xr, self.dr) = sems
        self.small = small
        self.small_sems = small_sems
        self.half, self.private, self.shared = split_rows(rows, self.X)

    def turn(self, t):
        block, r = (t - 1) // self.B, lax.rem(t - 1 + self.B, self.B)
        r = r + jnp.where(block == self.A - 1, 1, 0)
        near = jnp.where(r == 0, block + 1, r * self.A + block)
        if self.B == 2 and self.A > 2:
            near = jnp.where(self.middle & (t == 2), 2, jnp.where(self.middle & (t == 3), self.A, near))
            near = jnp.where(self.middle & (t == 4), 3, jnp.where(self.middle & (t == 5), self.A + 1, near))
        return jnp.where(t == 0, 0, near)

    def shard(self, t):
        i = self.turn(t)
        a = column(self.a, lax.rem(i, self.A), self.A)
        return a * self.B + lax.rem(self.b - i // self.A + self.B, self.B)

    def window(self, s, core):
        start = self.base + core * self.half + self.x * self.private
        return self.buf.at[s, pl.ds(pl.multiple_of(start, PACK), self.private + self.shared)]

    def own(self, s, core, plane):
        start = self.base + core * self.half + plane * (self.private + self.shared)
        return self.buf.at[s, pl.ds(pl.multiple_of(start, PACK), self.private)]

    def copy(self, ref, send, recv, **to):
        return pltpu.make_async_remote_copy(
            src_ref=ref, dst_ref=ref, send_sem=send, recv_sem=recv,
            device_id=to, device_id_type=MESH,
        )

    def along(self, p, way):
        s = p * self.B + self.b
        to = self.a + 1 - 2 * way
        out = []
        if self.small is not None:
            zs, _, wr = self.small_sems
            out.append(self.copy(self.small.at[s], zs.at[way, p], wr.at[s], a=to))
        out.append(self.copy(self.window(s, self.c), self.zs.at[self.w, way, p], self.wr.at[self.w, s], a=to))
        return out

    def across(self, p, k):
        s = p * self.B + self.b
        to = lax.rem(self.b + k, self.B)
        out = []
        if self.small is not None:
            _, ys, wr = self.small_sems
            out.append(self.copy(self.small.at[s], ys.at[k, p], wr.at[s], b=to))
        out.append(self.copy(self.window(s, self.c), self.ys.at[self.w, k, p], self.wr.at[self.w, s], b=to))
        return out

    def plane(self, s, k):
        return self.copy(
            self.own(s, self.c, self.x), self.xs.at[self.w, k, s],
            self.xr.at[self.w, k, s], x=lax.rem(self.x + k, self.X),
        )

    def from_plane(self, s, k):
        ref = self.own(s, self.c, lax.rem(self.x - k + self.X, self.X))
        return self.copy(ref, self.xs.at[self.w, k, s], self.xr.at[self.w, k, s], x=self.x)

    def pair(self, s, e, core):
        if e == 0:
            ref = self.window(s, core)
        else:
            ref = self.own(s, core, lax.rem(self.x - e + self.X, self.X))
        return self.copy(ref, self.ds.at[self.w, e, s], self.dr.at[self.w, e, s], c=1 - self.c)

    def sends(self, p, right, left, run):
        @pl.when(right & (self.a + 1 < self.A))
        def _():
            run(self.along(p, 0))

        @pl.when(left & (self.a > 0))
        def _():
            run(self.along(p, 1))

    @staticmethod
    def start(copies):
        for copy in copies:
            copy.start()

    @staticmethod
    def sent(copies):
        for copy in copies:
            copy.wait_send()

    def begin_line(self):
        self.sends(self.a, self.a >= 0, self.a >= 0, self.start)

    def begin_side(self):
        for k in range(1, self.B):
            self.start(self.across(self.a, k))

    def own_sent(self):
        self.settled = True
        self.sends(self.a, self.a >= 0, self.a >= 0, self.sent)
        for k in range(1, self.B):
            self.sent(self.across(self.a, k))

    def relay(self, t):
        s = self.shard(t)
        p = s // self.B
        if self.small is not None:
            zs, _, wr = self.small_sems
            self.copy(self.small.at[s], zs.at[0, 0], wr.at[s], c=self.c).wait_recv()
        self.copy(self.window(s, self.c), self.zs.at[self.w, 0, 0], self.wr.at[self.w, s], c=self.c).wait_recv()

        @pl.when(lax.rem(s, self.B) == self.b)
        def _():
            self.sends(p, p < self.a, p > self.a, self.start)
            for k in range(1, self.B):
                self.start(self.across(p, k))

        for k in range(1, self.X):
            self.plane(s, k).start()
        self.pair(s, 0, self.c).start()

    def relay_plane(self, i):
        s = self.shard(i)
        for k in range(1, self.X):
            self.from_plane(s, k).wait_recv()
            self.pair(s, k, self.c).start()

    def ready(self, i):
        s = self.shard(i)
        for e in range(self.X):
            self.pair(s, e, 1 - self.c).wait_recv()

    def drain(self):
        def line(p, _):
            @pl.when((p != self.a) | (not self.settled))
            def _():
                self.sends(p, p <= self.a, p >= self.a, self.sent)
                for k in range(1, self.B):
                    self.sent(self.across(p, k))

            return 0

        lax.fori_loop(0, self.A, line, 0)

        def one(i, _):
            s = self.shard(i)
            for k in range(1, self.X):
                self.plane(s, k).wait_send()
            for e in range(self.X):
                self.pair(s, e, self.c).wait_send()
            return 0

        lax.fori_loop(1, self.A * self.B, one, 0)


def scan_tokens(st, dr, bx, rate, hidden, tokens, tiles, each=None):
    rates = [[rate[8 * k : 8 * k + 8, cols] for cols in tiles] for k in range(2)]
    count = len(tiles)

    def body(i, carry):
        h = [list(carry[:count]), list(carry[count:])]
        for u in range(STEP):
            at = pl.multiple_of((i * STEP + u) * 16, 16)
            b = [bx[pl.ds(at + 8 * k, 8), :] for k in range(2)]
            block = i * (STEP // ROWS8) + u // ROWS8
            row = slice(u % ROWS8, u % ROWS8 + 1)
            for j, cols in enumerate(tiles):
                s = jnp.broadcast_to(st[block, row, cols], (ROWS8, LANES))
                d = jnp.broadcast_to(dr[block, row, cols], (ROWS8, LANES))
                for k in range(2):
                    h[k][j] = jnp.exp2(s * rates[k][j]) * h[k][j] + b[k] * d
            if each is not None:
                each(i, u, at, h)
        return tuple(h[0]) + tuple(h[1])

    return lax.fori_loop(0, tokens // STEP, body, hidden)


def silu(v):
    half = 0.5 * v
    return half + half * jnp.tanh(half)


def mixer_kernel(
    sizes, states,
    x_hbm, g_hbm, xw_hbm, dtw_hbm, cw_ref, cb_ref, db_ref, sk_ref, al_ref, gain_ref,
    gv,
    xv, xwv, dtv, last, halo_out, halo, cp, w1, w2, acc, nm, bx, cx, st, dr, rt, zb,
    eb, rb, sb, h0b,
    lsem, hsem, cz, cy, cr,
    zs, ys, xs, ds, wr, xr, dr_sem,
    es, er, bs, br,
):
    A, B, X = sizes
    D = A * B
    tokens, inner = xv.shape
    wide, shard = xwv.shape
    nb = shard // WIDE
    rank = gain_ref.shape[1]
    taps = cw_ref.shape[0]
    groups = inner // GROUP
    span = rank + 3 * PACK
    cuts = pieces_of(nb)
    part_blocks = nb // cuts
    rows1, rows2 = w1.shape[1] // cuts, w2.shape[1] // cuts
    spot1 = lambda j: (j // part_blocks) * rows1 + (j % part_blocks) * wide
    spot2 = lambda j: (j // part_blocks) * rows2 + (j % part_blocks) * span
    a, b, x, c = (lax.axis_index(n) for n in ("a", "b", "x", "c"))
    me = a * B + b
    place = (a, b, x, c)
    sems = (zs, ys, xs, ds, wr, xr, dr_sem)

    loads = [
        pltpu.make_async_copy(src, dst, lsem.at[n])
        for n, (src, dst) in enumerate(((xw_hbm, xwv), (dtw_hbm, dtv), (x_hbm, xv), (g_hbm, gv), (x_hbm.at[pl.ds(tokens - ROWS8, ROWS8)], last)))
    ]
    for n in (4, 0, 1, 2, 3):
        loads[n].start()

    barrier = pltpu.get_barrier_semaphore()
    for r in range(1, D):
        other = lax.rem(me + r, D)
        pl.semaphore_signal(
            barrier, inc=1, device_id={"a": other // B, "b": lax.rem(other, B)}, device_id_type=MESH
        )
    for k in range(1, X):
        pl.semaphore_signal(barrier, inc=1, device_id={"x": lax.rem(x + k, X)}, device_id_type=MESH)
    pl.semaphore_signal(barrier, inc=1, device_id={"c": 1 - c}, device_id_type=MESH)

    lanes = cb_ref[...].astype(F32)
    per = WIDE // LANES
    bias = lambda j: jnp.concatenate([lanes[n : n + 1] for n in range(per * j, per * j + per)], 1)
    weight = cw_ref[...].astype(F32)
    pieces = [r for j in range(nb) for r in (weight[:, WIDE * j : WIDE * j + WIDE], bias(j))]
    fill = cp.shape[1] - (taps + 1) * nb
    cp[me] = jnp.concatenate(pieces + [jnp.zeros((fill, WIDE), F32)], 0).astype(BF16)
    loads[4].wait()
    tail = last[...].astype(F32)
    fill = halo.shape[1] - (taps - 1) * nb
    for s in range(D):
        pieces = [
            tail[ROWS8 - taps + 1 :, n : n + WIDE] for n in range(s * shard, s * shard + shard, WIDE)
        ]
        halo_out[s] = jnp.concatenate(pieces + [jnp.zeros((fill, WIDE), F32)], 0).astype(BF16)
    loads[0].wait()
    for j in range(nb):
        w1[me, spot1(j) : spot1(j) + wide, :] = xwv[:, WIDE * j : WIDE * j + WIDE]
    with jax.named_scope("barrier"):
        pl.semaphore_wait(barrier, D - 1 + X - 1 + 1)

    after = lax.rem(me + 1, D)
    halo_copy = pltpu.make_async_remote_copy(
        src_ref=halo_out, dst_ref=halo, send_sem=hsem.at[0], recv_sem=hsem.at[1],
        device_id={"a": after // B, "b": lax.rem(after, B)}, device_id_type=MESH,
    )
    first = [
        Gather(sizes, place, n, w1, n * rows1, rows1, sems, *((cp, (cz, cy, cr)) if n == 0 else ()))
        for n in range(cuts)
    ]
    second = [Gather(sizes, place, cuts + n, w2, n * rows2, rows2, sems) for n in range(cuts)]
    halo_copy.start()
    for n, g in enumerate(first):
        if n >= AHEAD:
            first[n - AHEAD].own_sent()
        g.begin_line()
        g.begin_side()

    for j in range(nb):
        cols = slice(WIDE * j, WIDE * j + WIDE)
        rate = -jnp.exp(al_ref[:, cols]) * LOG2E
        high = rate.astype(BF16)
        base = spot2(j) + rank
        w2[me, base : base + states, :] = high
        w2[me, base + PACK : base + PACK + states, :] = (rate - high.astype(F32)).astype(BF16)
        two = jnp.concatenate([db_ref[:, cols], sk_ref[:, cols]], 0)
        top = two.astype(BF16).astype(F32)
        w2[me, base + 2 * PACK : base + 3 * PACK, :] = jnp.concatenate(
            [top, two - top, jnp.zeros((PACK - 4, WIDE), F32)], 0
        ).astype(BF16)
    loads[1].wait()
    for j in range(nb):
        w2[me, spot2(j) : spot2(j) + rank, :] = dtv[:, WIDE * j : WIDE * j + WIDE]
    loads[2].wait()
    acc[...] = jnp.zeros_like(acc)
    lead = (me > 0).astype(F32)
    shard_at = first[0].shard

    def convolve(i):
        s = shard_at(i)
        weight = cp[s].astype(F32)
        before = halo[s].astype(F32) * lead
        for j in range(nb):
            cols = pl.ds(pl.multiple_of(s * shard + WIDE * j, WIDE), WIDE)
            row = lambda n: weight[(taps + 1) * j + n : (taps + 1) * j + n + 1]
            cur = xv[:, cols].astype(F32)
            head = before[(taps - 1) * j : (taps - 1) * (j + 1)]
            ext = jnp.concatenate([jnp.zeros((ROWS8 - taps + 1, WIDE), F32), head, cur], 0)
            total = row(taps) + row(taps - 1) * cur
            for tap in range(taps - 1):
                low = ROWS8 - taps + 1 + tap
                total = total + row(tap) * ext[low : low + tokens]
            xv[:, cols] = silu(total).astype(BF16)

    def project(i):
        s = shard_at(i)
        if not isinstance(i, int) or i > 0:
            for g in first:
                g.ready(i)
        total = acc[...]
        for j in range(nb):
            cols = pl.ds(pl.multiple_of(s * shard + WIDE * j, WIDE), WIDE)
            total = total + lax.dot_general(
                xv[:, cols], w1[s, spot1(j) : spot1(j) + wide, :], (((1,), (1,)), ((), ())),
                preferred_element_type=F32,
            )
        acc[...] = total

    def step_first(t, _):
        for g in first:
            g.relay(t)

        @pl.when(t > 3)
        def _():
            for g in first:
                g.relay_plane(t - 3)

        @pl.when(t == 1)
        def _():
            halo_copy.wait_recv()

        convolve(t - 1)

        @pl.when(t > 5)
        def _():
            project(t - 5)

        return 0

    split = (A - 2) * B + 2
    with jax.named_scope("w1a"):
        lax.fori_loop(1, split, step_first, 0)
        for w in second:
            w.begin_line()
        lax.fori_loop(split, D, step_first, 0)
        for w in second:
            w.begin_side()
    middle = second[0].middle

    def second_relay(t, when):
        @pl.when(when)
        def _():
            for w in second:
                w.relay(t)

    with jax.named_scope("w1b"):
        convolve(D - 1)
        for t in (D - 3, D - 2):
            for g in first:
                g.relay_plane(t)
        project(0)
        for w in second:
            w.relay(1)
        second_relay(2, middle)
        for g in first:
            g.relay_plane(D - 1)
        for t in range(D - 5, D):
            project(t)

    with jax.named_scope("norm"):
        low = acc[:, :rank]
        nm[...] = (
            low * lax.rsqrt(jnp.mean(low * low, axis=1, keepdims=True) + 1e-06) * gain_ref[...]
        ).astype(BF16)
        bc = acc[:, rank:]
        for n in range(states):
            at = pl.ds(n, tokens, stride=states)
            bx[at, :] = jnp.broadcast_to(bc[:, n : n + 1], (tokens, LANES))
            cx[at, :] = jnp.broadcast_to(bc[:, states + n : states + n + 1], (tokens, LANES))
        second_relay(2, jnp.logical_not(middle))
        for w in second:
            w.relay_plane(1)

    tiles = GROUP // LANES
    blocks = GROUP // WIDE
    local_order = groups == D

    def strips(part):
        return [slice(LANES * j, LANES * j + LANES) for j in range(part, part + TILES)]

    def group_at(i):
        return shard_at(i) if local_order else i

    def to_combiner(g):
        return pltpu.make_async_remote_copy(
            src_ref=eb.at[g], dst_ref=rb.at[me], send_sem=es.at[g], recv_sem=er.at[me],
            device_id={"a": g // B, "b": lax.rem(g, B)}, device_id_type=MESH,
        )

    def pass_one(i, _):
        if local_order:
            @pl.when(i + 3 < D)
            def _():
                for w in second:
                    w.relay(i + 3)

            @pl.when(i > 0)
            def _():
                for w in second:
                    w.ready(i)

        g = group_at(i)
        sums = []
        for q in range(blocks):
            cb = g * blocks + q
            s, j = cb // nb, lax.rem(cb, nb)
            cols = pl.ds(pl.multiple_of(cb * WIDE, WIDE), WIDE)
            base = pl.multiple_of(spot2(j), PACK)
            rows = lambda n: pl.ds(pl.multiple_of(base + rank + n * PACK, PACK), PACK)
            misc = w2[s, rows(2), :].astype(F32)
            rt[g, :, WIDE * q : WIDE * q + WIDE] = w2[s, rows(0), :].astype(F32) + w2[s, rows(1), :].astype(F32)
            raw = jnp.dot(nm[...], w2[s, pl.ds(base, rank), :], preferred_element_type=F32)
            raw = raw + (misc[0:1] + misc[2:3])
            small = jnp.exp2(jnp.abs(raw) * -LOG2E)
            step = jnp.maximum(raw, 0.0) + LN2 * jnp.log2(1.0 + small)
            st[:, :, cols] = step.reshape(tokens // ROWS8, ROWS8, WIDE)
            dr[:, :, cols] = (step * xv[:, cols].astype(F32)).reshape(tokens // ROWS8, ROWS8, WIDE)
            total = jnp.sum(step, axis=0, keepdims=True)
            sums += [total[:, :LANES], total[:, LANES:]]
        view = pl.ds(pl.multiple_of(g * GROUP, GROUP), GROUP)
        zero = jnp.zeros((ROWS8, LANES), F32)
        for part in range(0, tiles, TILES):
            h = scan_tokens(
                st.at[:, :, view], dr.at[:, :, view], bx, rt.at[g], (zero,) * (2 * TILES), tokens, strips(part)
            )
            if local_order and part == 0:
                @pl.when(i + 2 < D)
                def _():
                    with jax.named_scope("pl"):
                        for w in second:
                            w.relay_plane(i + 2)

            for j in range(TILES):
                n = 16 * (part + j)
                eb[g, n : n + 16, :] = jnp.concatenate([h[j], h[TILES + j]], 0).astype(BF16)
        sums = jnp.concatenate(sums, 0)
        top = sums.astype(BF16).astype(F32)
        eb[g, 16 * tiles : 16 * tiles + 16, :] = jnp.concatenate([top, sums - top], 0).astype(BF16)

        @pl.when(g != me)
        def _():
            to_combiner(g).start()

        @pl.when(g == me)
        def _():
            rb[me] = eb[me]

        return 0

    def settle(i, _):
        for w in second:
            @pl.when(i > 2)
            def _():
                w.relay(i)

            @pl.when(i > 1)
            def _():
                w.relay_plane(i)

            w.ready(i)
        return 0

    if not local_order:
        lax.fori_loop(1, D, settle, 0)
    with jax.named_scope("pass1"):
        lax.fori_loop(0, groups, pass_one, 0)

    def to_owner(k):
        return pltpu.make_async_remote_copy(
            src_ref=sb.at[k], dst_ref=h0b.at[me], send_sem=bs.at[k], recv_sem=br.at[me],
            device_id={"a": k // B, "b": lax.rem(k, B)}, device_id_type=MESH,
        )

    def arrival(k):
        return pltpu.make_async_remote_copy(
            src_ref=rb.at[k], dst_ref=rb.at[k], send_sem=es.at[0], recv_sem=er.at[k],
            device_id={"c": c}, device_id_type=MESH,
        )

    with jax.named_scope("drain"):
        for w in first + second:
            w.drain()

    with jax.named_scope("combine"):
        @pl.when(me < groups)
        def _():
            def combine(k, start):
                @pl.when(k != me)
                def _():
                    arrival(k).wait_recv()

                now = []
                both = rb[k, 16 * tiles : 16 * tiles + 16, :].astype(F32)
                sums = both[0:8] + both[8:16]
                for j in range(tiles):
                    sb[k, 16 * j : 16 * j + 16, :] = start[j].astype(BF16)
                    decay = jnp.exp2(sums[j : j + 1, :] * rt[me, :, LANES * j : LANES * j + LANES])
                    now.append(decay * start[j] + rb[k, 16 * j : 16 * j + 16, :].astype(F32))

                @pl.when(k != me)
                def _():
                    to_owner(k).start()

                @pl.when(k == me)
                def _():
                    h0b[me] = sb[me]

                return tuple(now)

            lax.fori_loop(0, D, combine, (jnp.zeros((16, LANES), F32),) * tiles)

    loads[3].wait()

    def start_of(g):
        return pltpu.make_async_remote_copy(
            src_ref=h0b.at[g], dst_ref=h0b.at[g], send_sem=bs.at[0], recv_sem=br.at[g],
            device_id={"c": c}, device_id_type=MESH,
        )

    def pass_two(i, _):
        g = lax.rem(me + i, groups)

        @pl.when(g != me)
        def _():
            start_of(g).wait_recv()

        view = pl.ds(pl.multiple_of(g * GROUP, GROUP), GROUP)
        xg, gg = xv.at[:, view], gv.at[:, view]
        direct = []
        for q in range(blocks):
            cb = g * blocks + q
            s, j = cb // nb, lax.rem(cb, nb)
            misc = w2[s, pl.ds(pl.multiple_of(spot2(j) + rank + 2 * PACK, PACK), PACK), :].astype(F32)
            both = misc[1:2] + misc[3:4]
            direct += [both[:, LANES * n : LANES * n + LANES] for n in range(WIDE // LANES)]
        for part in range(0, tiles, TILES):
            cols = strips(part)
            first_state = [h0b[g, 16 * j : 16 * j + 16, :].astype(F32) for j in range(part, part + TILES)]
            h = tuple(v[:8] for v in first_state) + tuple(v[8:] for v in first_state)

            def each(i, u, at, now):
                c0, c1 = (cx[pl.ds(at + 8 * k, 8), :] for k in range(2))
                for j in range(TILES):
                    n = PITCH * (STEP * j + u)
                    zb[n : n + 8, :] = c0 * now[0][j] + c1 * now[1][j]
                if u < STEP - 1:
                    return
                where = pl.ds(pl.multiple_of(i * STEP, STEP), STEP)
                for j in range(TILES):
                    halves = []
                    for t in range(0, STEP, 8):
                        o = [zb[pl.ds(PITCH * (STEP * j + t) + q, 8, stride=PITCH), :] for q in range(8)]
                        halves.append(((o[0] + o[1]) + (o[2] + o[3])) + ((o[4] + o[5]) + (o[6] + o[7])))
                    y = jnp.concatenate(halves, 0) + direct[part + j] * xg[where, cols[j]].astype(F32)
                    gg[where, cols[j]] = (y * silu(gg[where, cols[j]].astype(F32))).astype(BF16)

            scan_tokens(st.at[:, :, view], dr.at[:, :, view], bx, rt.at[g], h, tokens, cols, each)
        return 0

    with jax.named_scope("pass2"):
        lax.fori_loop(0, groups, pass_two, 0)

    def finish(g, _):

        @pl.when(g != me)
        def _():
            to_combiner(g).wait_send()

        return 0

    with jax.named_scope("finish"):
        lax.fori_loop(0, groups, finish, 0)

        @pl.when(me < groups)
        def _():
            def sent(k, _):
                @pl.when(k != me)
                def _():
                    to_owner(k).wait_send()

                return 0

            lax.fori_loop(0, D, sent, 0)

        halo_copy.wait_send()


def write_kernel(y_ref, out_hbm, sem):
    rows = y_ref.shape[0] // PARTS
    copies = [
        pltpu.make_async_copy(y_ref.at[pl.ds(n * rows, rows)], out_hbm.at[pl.ds(n * rows, rows)], sem.at[n])
        for n in range(PARTS)
    ]
    for copy in copies:
        copy.start()
    for copy in copies:
        copy.wait()


def local(sizes, conv_input, gate_input, conv_weight, conv_bias, x_weight, dt_gain, dt_weight, dt_bias, a_log, skip):
    A, B, X = sizes
    D = A * B
    tokens, inner = conv_input.shape
    rank, shard = dt_weight.shape
    states = a_log.shape[0]
    nb = shard // WIDE
    groups = inner // GROUP
    small = -(-(conv_weight.shape[0] + 1) * nb // PACK) * PACK
    edge = -(-(conv_weight.shape[0] - 1) * nb // PACK) * PACK
    cuts = pieces_of(nb)
    r1 = cuts * padded_rows(x_weight.shape[1] * nb // cuts, X)
    r2 = cuts * padded_rows((rank + 3 * PACK) * nb // cuts, X)
    tiles = GROUP // LANES
    packet = 16 * tiles + 16
    hbm = pl.BlockSpec(memory_space=pltpu.HBM)
    vmem = pl.BlockSpec(memory_space=pltpu.VMEM)
    dma = pltpu.SemaphoreType.DMA
    all_ = 2 * cuts
    mixed = pl.pallas_call(
        functools.partial(mixer_kernel, sizes, states),
        in_specs=[hbm] * 4 + [vmem] * 6,
        out_specs=vmem,
        out_shape=jax.ShapeDtypeStruct((tokens, inner), BF16),
        scratch_shapes=[
            pltpu.VMEM((tokens, inner), BF16),
            pltpu.VMEM((x_weight.shape[1], shard), BF16),
            pltpu.VMEM(dt_weight.shape, BF16),
            pltpu.VMEM((ROWS8, inner), BF16),
            pltpu.VMEM((D, edge, WIDE), BF16),
            pltpu.VMEM((D, edge, WIDE), BF16),
            pltpu.VMEM((D, small, WIDE), BF16),
            pltpu.VMEM((D, r1, WIDE), BF16),
            pltpu.VMEM((D, r2, WIDE), BF16),
            pltpu.VMEM((tokens, x_weight.shape[1]), F32),
            pltpu.VMEM((tokens, rank), BF16),
            pltpu.VMEM((tokens * states, LANES), F32),
            pltpu.VMEM((tokens * states, LANES), F32),
            pltpu.VMEM((tokens // ROWS8, ROWS8, inner), F32),
            pltpu.VMEM((tokens // ROWS8, ROWS8, inner), F32),
            pltpu.VMEM((groups, states, GROUP), F32),
            pltpu.VMEM((PITCH * STEP * TILES, LANES), F32),
            pltpu.VMEM((groups, packet, LANES), BF16),
            pltpu.VMEM((D, packet, LANES), BF16),
            pltpu.VMEM((D, 16 * tiles, LANES), BF16),
            pltpu.VMEM((groups, 16 * tiles, LANES), BF16),
            dma((5,)), dma((2,)), dma((2, A)), dma((B, A)), dma((D,)),
            dma((all_, 2, A)), dma((all_, B, A)), dma((all_, X, D)), dma((all_, X, D)),
            dma((all_, D)), dma((all_, X, D)), dma((all_, X, D)),
            dma((groups,)), dma((D,)), dma((D,)), dma((groups,)),
        ],
        compiler_params=pltpu.CompilerParams(
            collective_id=0, has_side_effects=True, vmem_limit_bytes=VMEM_MAIN
        ),
        name="mixer",
    )(
        *(
            pltpu.with_memory_space_constraint(v, pltpu.HBM)
            for v in (
                conv_input, gate_input, x_weight.T, dt_weight, conv_weight, conv_bias.reshape(-1, LANES),
                dt_bias[None, :], skip[None, :], a_log, dt_gain[None, :],
            )
        )
    )
    return pl.pallas_call(
        write_kernel,
        in_specs=[vmem],
        out_specs=hbm,
        out_shape=jax.ShapeDtypeStruct((tokens, inner), BF16),
        scratch_shapes=[dma((PARTS,))],
        compiler_params=pltpu.CompilerParams(vmem_limit_bytes=VMEM_COPY),
        name="write",
    )(mixed)


def solution(mesh):
    seq, batch = mesh.shape["seq"], mesh.shape["batch"]
    cores = 2
    A = math.gcd(seq, batch)
    B, X = seq // A, batch // cores
    grid = Mesh(mesh.devices.reshape(A, B, X, cores), ("a", "b", "x", "c"))
    seqs = ("a", "b")
    rows = P(("x", "c", "a", "b"), None)
    return jax.shard_map(
        functools.partial(local, (A, B, X)),
        mesh=grid,
        in_specs=(
            rows, rows, P(None, seqs), P(seqs), P(seqs, None), P(), P(None, seqs), P(seqs), P(None, seqs), P(seqs),
        ),
        out_specs=rows,
        check_vma=False,
    )
```

```python
import functools
import math

import jax
import jax.numpy as jnp
from jax import lax
from jax.experimental import pallas as pl
from jax.experimental.pallas import tpu as pltpu
from jax.sharding import Mesh
from jax.sharding import PartitionSpec as P

LOG2E = 1.4426950408889634
LN2 = 0.6931471805599453
LANES = 128
ROWS8 = 8
PACK = 16
WIDE = 256
GROUP = 1024
STEP = 64
TILES = 4
PITCH = 9
AHEAD = 9
CUTS = 2
SHARE = 0.34
PARTS = 4
VMEM_MAIN = 48 * 1024 * 1024
VMEM_COPY = 4 * 1024 * 1024
MESH = pl.DeviceIdType.MESH
F32 = jnp.float32
BF16 = jnp.bfloat16


def split_rows(rows, planes):
    half = rows // 2
    if planes == 2:
        private = round(half * SHARE / PACK) * PACK
        return half, private, half - 2 * private
    return half, half // planes, 0


def padded_rows(rows, planes):
    unit = 2 * PACK * (planes if planes > 2 else 1)
    return -(-rows // unit) * unit


def column(a, i, size):
    turn = lax.rem(i, 2)
    inner = a + (1 - 2 * turn) * ((i + 1) // 2)
    outer = jnp.where(2 * a < size - 1, i, size - 1 - i)
    return jnp.where(i <= 2 * jnp.minimum(a, size - 1 - a), inner, outer)


def pieces_of(blocks):
    return math.gcd(blocks, CUTS)


class Gather:
    def __init__(self, sizes, place, which, buf, base, rows, sems, small=None, small_sems=None):
        self.A, self.B, self.X = sizes
        self.a, self.b, self.x, self.c = place
        self.w = which
        self.buf = buf
        self.base = base
        self.settled = False
        self.middle = (self.a > 0) & (self.a + 1 < self.A)
        (self.zs, self.ys, self.xs, self.ds, self.wr, self.xr, self.dr) = sems
        self.small = small
        self.small_sems = small_sems
        self.half, self.private, self.shared = split_rows(rows, self.X)

    def turn(self, t):
        block, r = (t - 1) // self.B, lax.rem(t - 1 + self.B, self.B)
        r = r + jnp.where(block == self.A - 1, 1, 0)
        near = jnp.where(r == 0, block + 1, r * self.A + block)
        if self.B == 2 and self.A > 2:
            near = jnp.where(self.middle & (t == 2), 2, jnp.where(self.middle & (t == 3), self.A, near))
            near = jnp.where(self.middle & (t == 4), 3, jnp.where(self.middle & (t == 5), self.A + 1, near))
        return jnp.where(t == 0, 0, near)

    def shard(self, t):
        i = self.turn(t)
        a = column(self.a, lax.rem(i, self.A), self.A)
        return a * self.B + lax.rem(self.b - i // self.A + self.B, self.B)

    def window(self, s, core):
        start = self.base + core * self.half + self.x * self.private
        return self.buf.at[s, pl.ds(pl.multiple_of(start, PACK), self.private + self.shared)]

    def own(self, s, core, plane):
        start = self.base + core * self.half + plane * (self.private + self.shared)
        return self.buf.at[s, pl.ds(pl.multiple_of(start, PACK), self.private)]

    def copy(self, ref, send, recv, **to):
        return pltpu.make_async_remote_copy(
            src_ref=ref, dst_ref=ref, send_sem=send, recv_sem=recv,
            device_id=to, device_id_type=MESH,
        )

    def along(self, p, way):
        s = p * self.B + self.b
        to = self.a + 1 - 2 * way
        out = []
        if self.small is not None:
            zs, _, wr = self.small_sems
            out.append(self.copy(self.small.at[s], zs.at[way, p], wr.at[s], a=to))
        out.append(self.copy(self.window(s, self.c), self.zs.at[self.w, way, p], self.wr.at[self.w, s], a=to))
        return out

    def across(self, p, k):
        s = p * self.B + self.b
        to = lax.rem(self.b + k, self.B)
        out = []
        if self.small is not None:
            _, ys, wr = self.small_sems
            out.append(self.copy(self.small.at[s], ys.at[k, p], wr.at[s], b=to))
        out.append(self.copy(self.window(s, self.c), self.ys.at[self.w, k, p], self.wr.at[self.w, s], b=to))
        return out

    def plane(self, s, k):
        return self.copy(
            self.own(s, self.c, self.x), self.xs.at[self.w, k, s],
            self.xr.at[self.w, k, s], x=lax.rem(self.x + k, self.X),
        )

    def from_plane(self, s, k):
        ref = self.own(s, self.c, lax.rem(self.x - k + self.X, self.X))
        return self.copy(ref, self.xs.at[self.w, k, s], self.xr.at[self.w, k, s], x=self.x)

    def pair(self, s, e, core):
        if e == 0:
            ref = self.window(s, core)
        else:
            ref = self.own(s, core, lax.rem(self.x - e + self.X, self.X))
        return self.copy(ref, self.ds.at[self.w, e, s], self.dr.at[self.w, e, s], c=1 - self.c)

    def sends(self, p, right, left, run):
        @pl.when(right & (self.a + 1 < self.A))
        def _():
            run(self.along(p, 0))

        @pl.when(left & (self.a > 0))
        def _():
            run(self.along(p, 1))

    @staticmethod
    def start(copies):
        for copy in copies:
            copy.start()

    @staticmethod
    def sent(copies):
        for copy in copies:
            copy.wait_send()

    def begin_line(self):
        self.sends(self.a, self.a >= 0, self.a >= 0, self.start)

    def begin_side(self):
        for k in range(1, self.B):
            self.start(self.across(self.a, k))

    def own_sent(self):
        self.settled = True
        self.sends(self.a, self.a >= 0, self.a >= 0, self.sent)
        for k in range(1, self.B):
            self.sent(self.across(self.a, k))

    def relay(self, t):
        s = self.shard(t)
        p = s // self.B
        if self.small is not None:
            zs, _, wr = self.small_sems
            self.copy(self.small.at[s], zs.at[0, 0], wr.at[s], c=self.c).wait_recv()
        self.copy(self.window(s, self.c), self.zs.at[self.w, 0, 0], self.wr.at[self.w, s], c=self.c).wait_recv()

        @pl.when(lax.rem(s, self.B) == self.b)
        def _():
            self.sends(p, p < self.a, p > self.a, self.start)
            for k in range(1, self.B):
                self.start(self.across(p, k))

        for k in range(1, self.X):
            self.plane(s, k).start()
        self.pair(s, 0, self.c).start()

    def relay_plane(self, i):
        s = self.shard(i)
        for k in range(1, self.X):
            self.from_plane(s, k).wait_recv()
            self.pair(s, k, self.c).start()

    def ready(self, i):
        s = self.shard(i)
        for e in range(self.X):
            self.pair(s, e, 1 - self.c).wait_recv()

    def drain(self):
        def line(p, _):
            @pl.when((p != self.a) | (not self.settled))
            def _():
                self.sends(p, p <= self.a, p >= self.a, self.sent)
                for k in range(1, self.B):
                    self.sent(self.across(p, k))

            return 0

        lax.fori_loop(0, self.A, line, 0)

        def one(i, _):
            s = self.shard(i)
            for k in range(1, self.X):
                self.plane(s, k).wait_send()
            for e in range(self.X):
                self.pair(s, e, self.c).wait_send()
            return 0

        lax.fori_loop(1, self.A * self.B, one, 0)


def scan_tokens(st, dr, bx, rate, hidden, tokens, tiles, each=None):
    rates = [[rate[8 * k : 8 * k + 8, cols] for cols in tiles] for k in range(2)]
    count = len(tiles)

    def body(i, carry):
        h = [list(carry[:count]), list(carry[count:])]
        for u in range(STEP):
            at = pl.multiple_of((i * STEP + u) * 16, 16)
            b = [bx[pl.ds(at + 8 * k, 8), :] for k in range(2)]
            block = i * (STEP // ROWS8) + u // ROWS8
            row = slice(u % ROWS8, u % ROWS8 + 1)
            for j, cols in enumerate(tiles):
                s = jnp.broadcast_to(st[block, row, cols], (ROWS8, LANES))
                d = jnp.broadcast_to(dr[block, row, cols], (ROWS8, LANES))
                for k in range(2):
                    h[k][j] = jnp.exp2(s * rates[k][j]) * h[k][j] + b[k] * d
            if each is not None:
                each(i, u, at, h)
        return tuple(h[0]) + tuple(h[1])

    return lax.fori_loop(0, tokens // STEP, body, hidden)


def silu(v):
    half = 0.5 * v
    return half + half * jnp.tanh(half)


def mixer_kernel(
    sizes, states,
    x_hbm, g_hbm, xw_hbm, dtw_hbm, cw_hbm, cb_hbm, db_hbm, sk_hbm, al_hbm, gain_hbm,
    gv,
    xv, xwv, dtv, last, halo_out, halo, cp, w1, w2, acc, nm, bx, cx, st, dr, rt, zb,
    eb, rb, sb, h0b,
    cw_ref, cb_ref, db_ref, sk_ref, al_ref, gain_ref,
    lsem, ssem, hsem, cz, cy, cr,
    zs, ys, xs, ds, wr, xr, dr_sem,
    es, er, bs, br,
):
    A, B, X = sizes
    D = A * B
    tokens, inner = xv.shape
    wide, shard = xwv.shape
    nb = shard // WIDE
    rank = gain_ref.shape[1]
    taps = cw_ref.shape[0]
    groups = inner // GROUP
    span = rank + 3 * PACK
    cuts = pieces_of(nb)
    part_blocks = nb // cuts
    rows1, rows2 = w1.shape[1] // cuts, w2.shape[1] // cuts
    spot1 = lambda j: (j // part_blocks) * rows1 + (j % part_blocks) * wide
    spot2 = lambda j: (j // part_blocks) * rows2 + (j % part_blocks) * span
    a, b, x, c = (lax.axis_index(n) for n in ("a", "b", "x", "c"))
    me = a * B + b
    place = (a, b, x, c)
    sems = (zs, ys, xs, ds, wr, xr, dr_sem)

    barrier = pltpu.get_barrier_semaphore()
    for r in range(1, D):
        other = lax.rem(me + r, D)
        pl.semaphore_signal(
            barrier, inc=1, device_id={"a": other // B, "b": lax.rem(other, B)}, device_id_type=MESH
        )
    for k in range(1, X):
        pl.semaphore_signal(barrier, inc=1, device_id={"x": lax.rem(x + k, X)}, device_id_type=MESH)
    pl.semaphore_signal(barrier, inc=1, device_id={"c": 1 - c}, device_id_type=MESH)

    loads = [
        pltpu.make_async_copy(src, dst, lsem.at[n])
        for n, (src, dst) in enumerate(((xw_hbm, xwv), (dtw_hbm, dtv), (x_hbm, xv), (g_hbm, gv), (x_hbm.at[pl.ds(tokens - ROWS8, ROWS8)], last)))
    ]
    for n in (4, 0, 1, 2, 3):
        loads[n].start()

    smalls = [
        pltpu.make_async_copy(src, dst, ssem.at[n])
        for n, (src, dst) in enumerate((
            (cw_hbm, cw_ref), (cb_hbm, cb_ref), (db_hbm, db_ref), (sk_hbm, sk_ref), (al_hbm, al_ref),
            (gain_hbm, gain_ref),
        ))
    ]
    for load in smalls:
        load.start()

    for load in smalls[:2]:
        load.wait()
    lanes = cb_ref[...].astype(F32)
    per = WIDE // LANES
    bias = lambda j: jnp.concatenate([lanes[n : n + 1] for n in range(per * j, per * j + per)], 1)
    weight = cw_ref[...].astype(F32)
    pieces = [r for j in range(nb) for r in (weight[:, WIDE * j : WIDE * j + WIDE], bias(j))]
    fill = cp.shape[1] - (taps + 1) * nb
    cp[me] = jnp.concatenate(pieces + [jnp.zeros((fill, WIDE), F32)], 0).astype(BF16)
    loads[4].wait()
    tail = last[...].astype(F32)
    fill = halo.shape[1] - (taps - 1) * nb
    for s in range(D):
        pieces = [
            tail[ROWS8 - taps + 1 :, n : n + WIDE] for n in range(s * shard, s * shard + shard, WIDE)
        ]
        halo_out[s] = jnp.concatenate(pieces + [jnp.zeros((fill, WIDE), F32)], 0).astype(BF16)
    loads[0].wait()
    for j in range(nb):
        w1[me, spot1(j) : spot1(j) + wide, :] = xwv[:, WIDE * j : WIDE * j + WIDE]
    with jax.named_scope("barrier"):
        pl.semaphore_wait(barrier, D - 1 + X - 1 + 1)

    after = lax.rem(me + 1, D)
    halo_copy = pltpu.make_async_remote_copy(
        src_ref=halo_out, dst_ref=halo, send_sem=hsem.at[0], recv_sem=hsem.at[1],
        device_id={"a": after // B, "b": lax.rem(after, B)}, device_id_type=MESH,
    )
    first = [
        Gather(sizes, place, n, w1, n * rows1, rows1, sems, *((cp, (cz, cy, cr)) if n == 0 else ()))
        for n in range(cuts)
    ]
    second = [Gather(sizes, place, cuts + n, w2, n * rows2, rows2, sems) for n in range(cuts)]
    halo_copy.start()
    for n, g in enumerate(first):
        if n >= AHEAD:
            first[n - AHEAD].own_sent()
        g.begin_line()
        g.begin_side()

    for load in smalls[2:]:
        load.wait()
    for j in range(nb):
        cols = slice(WIDE * j, WIDE * j + WIDE)
        rate = -jnp.exp(al_ref[:, cols]) * LOG2E
        high = rate.astype(BF16)
        base = spot2(j) + rank
        w2[me, base : base + states, :] = high
        w2[me, base + PACK : base + PACK + states, :] = (rate - high.astype(F32)).astype(BF16)
        two = jnp.concatenate([db_ref[:, cols], sk_ref[:, cols]], 0)
        top = two.astype(BF16).astype(F32)
        w2[me, base + 2 * PACK : base + 3 * PACK, :] = jnp.concatenate(
            [top, two - top, jnp.zeros((PACK - 4, WIDE), F32)], 0
        ).astype(BF16)
    loads[1].wait()
    for j in range(nb):
        w2[me, spot2(j) : spot2(j) + rank, :] = dtv[:, WIDE * j : WIDE * j + WIDE]
    loads[2].wait()
    acc[...] = jnp.zeros_like(acc)
    lead = (me > 0).astype(F32)
    shard_at = first[0].shard

    def convolve(i):
        s = shard_at(i)
        weight = cp[s].astype(F32)
        before = halo[s].astype(F32) * lead
        for j in range(nb):
            cols = pl.ds(pl.multiple_of(s * shard + WIDE * j, WIDE), WIDE)
            row = lambda n: weight[(taps + 1) * j + n : (taps + 1) * j + n + 1]
            cur = xv[:, cols].astype(F32)
            head = before[(taps - 1) * j : (taps - 1) * (j + 1)]
            ext = jnp.concatenate([jnp.zeros((ROWS8 - taps + 1, WIDE), F32), head, cur], 0)
            total = row(taps) + row(taps - 1) * cur
            for tap in range(taps - 1):
                low = ROWS8 - taps + 1 + tap
                total = total + row(tap) * ext[low : low + tokens]
            xv[:, cols] = silu(total).astype(BF16)

    def project(i):
        s = shard_at(i)
        if not isinstance(i, int) or i > 0:
            for g in first:
                g.ready(i)
        total = acc[...]
        for j in range(nb):
            cols = pl.ds(pl.multiple_of(s * shard + WIDE * j, WIDE), WIDE)
            total = total + lax.dot_general(
                xv[:, cols], w1[s, spot1(j) : spot1(j) + wide, :], (((1,), (1,)), ((), ())),
                preferred_element_type=F32,
            )
        acc[...] = total

    def step_first(t, _):
        for g in first:
            g.relay(t)

        @pl.when(t > 3)
        def _():
            for g in first:
                g.relay_plane(t - 3)

        @pl.when(t == 1)
        def _():
            halo_copy.wait_recv()

        convolve(t - 1)

        @pl.when(t > 5)
        def _():
            project(t - 5)

        return 0

    split = (A - 2) * B + 2
    with jax.named_scope("w1a"):
        lax.fori_loop(1, split, step_first, 0)
        for w in second:
            w.begin_line()
        lax.fori_loop(split, D, step_first, 0)
        for w in second:
            w.begin_side()
    middle = second[0].middle

    def second_relay(t, when):
        @pl.when(when)
        def _():
            for w in second:
                w.relay(t)

    with jax.named_scope("w1b"):
        convolve(D - 1)
        for t in (D - 3, D - 2):
            for g in first:
                g.relay_plane(t)
        project(0)
        for w in second:
            w.relay(1)
        second_relay(2, middle)
        for g in first:
            g.relay_plane(D - 1)
        for t in range(D - 5, D):
            project(t)

    with jax.named_scope("norm"):
        low = acc[:, :rank]
        nm[...] = (
            low * lax.rsqrt(jnp.mean(low * low, axis=1, keepdims=True) + 1e-06) * gain_ref[...]
        ).astype(BF16)
        bc = acc[:, rank:]
        for n in range(states):
            at = pl.ds(n, tokens, stride=states)
            bx[at, :] = jnp.broadcast_to(bc[:, n : n + 1], (tokens, LANES))
            cx[at, :] = jnp.broadcast_to(bc[:, states + n : states + n + 1], (tokens, LANES))
        second_relay(2, jnp.logical_not(middle))
        for w in second:
            w.relay_plane(1)

    tiles = GROUP // LANES
    blocks = GROUP // WIDE
    local_order = groups == D

    def strips(part):
        return [slice(LANES * j, LANES * j + LANES) for j in range(part, part + TILES)]

    def group_at(i):
        return shard_at(i) if local_order else i

    def to_combiner(g):
        return pltpu.make_async_remote_copy(
            src_ref=eb.at[g], dst_ref=rb.at[me], send_sem=es.at[g], recv_sem=er.at[me],
            device_id={"a": g // B, "b": lax.rem(g, B)}, device_id_type=MESH,
        )

    def pass_one(i, _):
        if local_order:
            @pl.when(i + 3 < D)
            def _():
                for w in second:
                    w.relay(i + 3)

            @pl.when(i > 0)
            def _():
                for w in second:
                    w.ready(i)

        g = group_at(i)
        sums = []
        for q in range(blocks):
            cb = g * blocks + q
            s, j = cb // nb, lax.rem(cb, nb)
            cols = pl.ds(pl.multiple_of(cb * WIDE, WIDE), WIDE)
            base = pl.multiple_of(spot2(j), PACK)
            rows = lambda n: pl.ds(pl.multiple_of(base + rank + n * PACK, PACK), PACK)
            misc = w2[s, rows(2), :].astype(F32)
            rt[g, :, WIDE * q : WIDE * q + WIDE] = w2[s, rows(0), :].astype(F32) + w2[s, rows(1), :].astype(F32)
            raw = jnp.dot(nm[...], w2[s, pl.ds(base, rank), :], preferred_element_type=F32)
            raw = raw + (misc[0:1] + misc[2:3])
            small = jnp.exp2(jnp.abs(raw) * -LOG2E)
            step = jnp.maximum(raw, 0.0) + LN2 * jnp.log2(1.0 + small)
            st[:, :, cols] = step.reshape(tokens // ROWS8, ROWS8, WIDE)
            dr[:, :, cols] = (step * xv[:, cols].astype(F32)).reshape(tokens // ROWS8, ROWS8, WIDE)
            total = jnp.sum(step, axis=0, keepdims=True)
            sums += [total[:, :LANES], total[:, LANES:]]
        view = pl.ds(pl.multiple_of(g * GROUP, GROUP), GROUP)
        zero = jnp.zeros((ROWS8, LANES), F32)
        for part in range(0, tiles, TILES):
            h = scan_tokens(
                st.at[:, :, view], dr.at[:, :, view], bx, rt.at[g], (zero,) * (2 * TILES), tokens, strips(part)
            )
            if local_order and part == 0:
                @pl.when(i + 2 < D)
                def _():
                    with jax.named_scope("pl"):
                        for w in second:
                            w.relay_plane(i + 2)

            for j in range(TILES):
                n = 16 * (part + j)
                eb[g, n : n + 16, :] = jnp.concatenate([h[j], h[TILES + j]], 0).astype(BF16)
        sums = jnp.concatenate(sums, 0)
        top = sums.astype(BF16).astype(F32)
        eb[g, 16 * tiles : 16 * tiles + 16, :] = jnp.concatenate([top, sums - top], 0).astype(BF16)

        @pl.when(g != me)
        def _():
            to_combiner(g).start()

        @pl.when(g == me)
        def _():
            rb[me] = eb[me]

        return 0

    def settle(i, _):
        for w in second:
            @pl.when(i > 2)
            def _():
                w.relay(i)

            @pl.when(i > 1)
            def _():
                w.relay_plane(i)

            w.ready(i)
        return 0

    if not local_order:
        lax.fori_loop(1, D, settle, 0)
    with jax.named_scope("pass1"):
        lax.fori_loop(0, groups, pass_one, 0)

    def to_owner(k):
        return pltpu.make_async_remote_copy(
            src_ref=sb.at[k], dst_ref=h0b.at[me], send_sem=bs.at[k], recv_sem=br.at[me],
            device_id={"a": k // B, "b": lax.rem(k, B)}, device_id_type=MESH,
        )

    def arrival(k):
        return pltpu.make_async_remote_copy(
            src_ref=rb.at[k], dst_ref=rb.at[k], send_sem=es.at[0], recv_sem=er.at[k],
            device_id={"c": c}, device_id_type=MESH,
        )

    with jax.named_scope("drain"):
        for w in first + second:
            w.drain()

    with jax.named_scope("combine"):
        @pl.when(me < groups)
        def _():
            def combine(k, start):
                @pl.when(k != me)
                def _():
                    arrival(k).wait_recv()

                now = []
                both = rb[k, 16 * tiles : 16 * tiles + 16, :].astype(F32)
                sums = both[0:8] + both[8:16]
                for j in range(tiles):
                    sb[k, 16 * j : 16 * j + 16, :] = start[j].astype(BF16)
                    decay = jnp.exp2(sums[j : j + 1, :] * rt[me, :, LANES * j : LANES * j + LANES])
                    now.append(decay * start[j] + rb[k, 16 * j : 16 * j + 16, :].astype(F32))

                @pl.when(k != me)
                def _():
                    to_owner(k).start()

                @pl.when(k == me)
                def _():
                    h0b[me] = sb[me]

                return tuple(now)

            lax.fori_loop(0, D, combine, (jnp.zeros((16, LANES), F32),) * tiles)

    loads[3].wait()

    def start_of(g):
        return pltpu.make_async_remote_copy(
            src_ref=h0b.at[g], dst_ref=h0b.at[g], send_sem=bs.at[0], recv_sem=br.at[g],
            device_id={"c": c}, device_id_type=MESH,
        )

    def pass_two(i, _):
        g = lax.rem(me + i, groups)

        @pl.when(g != me)
        def _():
            start_of(g).wait_recv()

        view = pl.ds(pl.multiple_of(g * GROUP, GROUP), GROUP)
        xg, gg = xv.at[:, view], gv.at[:, view]
        direct = []
        for q in range(blocks):
            cb = g * blocks + q
            s, j = cb // nb, lax.rem(cb, nb)
            misc = w2[s, pl.ds(pl.multiple_of(spot2(j) + rank + 2 * PACK, PACK), PACK), :].astype(F32)
            both = misc[1:2] + misc[3:4]
            direct += [both[:, LANES * n : LANES * n + LANES] for n in range(WIDE // LANES)]
        for part in range(0, tiles, TILES):
            cols = strips(part)
            first_state = [h0b[g, 16 * j : 16 * j + 16, :].astype(F32) for j in range(part, part + TILES)]
            h = tuple(v[:8] for v in first_state) + tuple(v[8:] for v in first_state)

            def each(i, u, at, now):
                c0, c1 = (cx[pl.ds(at + 8 * k, 8), :] for k in range(2))
                for j in range(TILES):
                    n = PITCH * (STEP * j + u)
                    zb[n : n + 8, :] = c0 * now[0][j] + c1 * now[1][j]
                if u < STEP - 1:
                    return
                where = pl.ds(pl.multiple_of(i * STEP, STEP), STEP)
                for j in range(TILES):
                    halves = []
                    for t in range(0, STEP, 8):
                        o = [zb[pl.ds(PITCH * (STEP * j + t) + q, 8, stride=PITCH), :] for q in range(8)]
                        halves.append(((o[0] + o[1]) + (o[2] + o[3])) + ((o[4] + o[5]) + (o[6] + o[7])))
                    y = jnp.concatenate(halves, 0) + direct[part + j] * xg[where, cols[j]].astype(F32)
                    gg[where, cols[j]] = (y * silu(gg[where, cols[j]].astype(F32))).astype(BF16)

            scan_tokens(st.at[:, :, view], dr.at[:, :, view], bx, rt.at[g], h, tokens, cols, each)
        return 0

    with jax.named_scope("pass2"):
        lax.fori_loop(0, groups, pass_two, 0)

    def finish(g, _):

        @pl.when(g != me)
        def _():
            to_combiner(g).wait_send()

        return 0

    with jax.named_scope("finish"):
        lax.fori_loop(0, groups, finish, 0)

        @pl.when(me < groups)
        def _():
            def sent(k, _):
                @pl.when(k != me)
                def _():
                    to_owner(k).wait_send()

                return 0

            lax.fori_loop(0, D, sent, 0)

        halo_copy.wait_send()


def write_kernel(y_ref, out_hbm, sem):
    rows = y_ref.shape[0] // PARTS
    copies = [
        pltpu.make_async_copy(y_ref.at[pl.ds(n * rows, rows)], out_hbm.at[pl.ds(n * rows, rows)], sem.at[n])
        for n in range(PARTS)
    ]
    for copy in copies:
        copy.start()
    for copy in copies:
        copy.wait()


def local(sizes, conv_input, gate_input, conv_weight, conv_bias, x_weight, dt_gain, dt_weight, dt_bias, a_log, skip):
    A, B, X = sizes
    D = A * B
    tokens, inner = conv_input.shape
    rank, shard = dt_weight.shape
    states = a_log.shape[0]
    nb = shard // WIDE
    groups = inner // GROUP
    small = -(-(conv_weight.shape[0] + 1) * nb // PACK) * PACK
    edge = -(-(conv_weight.shape[0] - 1) * nb // PACK) * PACK
    cuts = pieces_of(nb)
    r1 = cuts * padded_rows(x_weight.shape[1] * nb // cuts, X)
    r2 = cuts * padded_rows((rank + 3 * PACK) * nb // cuts, X)
    tiles = GROUP // LANES
    packet = 16 * tiles + 16
    hbm = pl.BlockSpec(memory_space=pltpu.HBM)
    vmem = pl.BlockSpec(memory_space=pltpu.VMEM)
    dma = pltpu.SemaphoreType.DMA
    all_ = 2 * cuts
    small_inputs = (
        conv_weight, conv_bias.reshape(-1, LANES), dt_bias[None, :], skip[None, :], a_log, dt_gain[None, :],
    )
    mixed = pl.pallas_call(
        functools.partial(mixer_kernel, sizes, states),
        in_specs=[hbm] * 10,
        out_specs=vmem,
        out_shape=jax.ShapeDtypeStruct((tokens, inner), BF16),
        scratch_shapes=[
            pltpu.VMEM((tokens, inner), BF16),
            pltpu.VMEM((x_weight.shape[1], shard), BF16),
            pltpu.VMEM(dt_weight.shape, BF16),
            pltpu.VMEM((ROWS8, inner), BF16),
            pltpu.VMEM((D, edge, WIDE), BF16),
            pltpu.VMEM((D, edge, WIDE), BF16),
            pltpu.VMEM((D, small, WIDE), BF16),
            pltpu.VMEM((D, r1, WIDE), BF16),
            pltpu.VMEM((D, r2, WIDE), BF16),
            pltpu.VMEM((tokens, x_weight.shape[1]), F32),
            pltpu.VMEM((tokens, rank), BF16),
            pltpu.VMEM((tokens * states, LANES), F32),
            pltpu.VMEM((tokens * states, LANES), F32),
            pltpu.VMEM((tokens // ROWS8, ROWS8, inner), F32),
            pltpu.VMEM((tokens // ROWS8, ROWS8, inner), F32),
            pltpu.VMEM((groups, states, GROUP), F32),
            pltpu.VMEM((PITCH * STEP * TILES, LANES), F32),
            pltpu.VMEM((groups, packet, LANES), BF16),
            pltpu.VMEM((D, packet, LANES), BF16),
            pltpu.VMEM((D, 16 * tiles, LANES), BF16),
            pltpu.VMEM((groups, 16 * tiles, LANES), BF16),
            *(pltpu.VMEM(v.shape, v.dtype) for v in small_inputs),
            dma((5,)), dma((len(small_inputs),)), dma((2,)), dma((2, A)), dma((B, A)), dma((D,)),
            dma((all_, 2, A)), dma((all_, B, A)), dma((all_, X, D)), dma((all_, X, D)),
            dma((all_, D)), dma((all_, X, D)), dma((all_, X, D)),
            dma((groups,)), dma((D,)), dma((D,)), dma((groups,)),
        ],
        compiler_params=pltpu.CompilerParams(
            collective_id=0, has_side_effects=True, vmem_limit_bytes=VMEM_MAIN
        ),
        name="mixer",
    )(
        *(
            pltpu.with_memory_space_constraint(v, pltpu.HBM)
            for v in (
                conv_input, gate_input, x_weight.T, dt_weight, *small_inputs
            )
        )
    )
    return pl.pallas_call(
        write_kernel,
        in_specs=[vmem],
        out_specs=hbm,
        out_shape=jax.ShapeDtypeStruct((tokens, inner), BF16),
        scratch_shapes=[dma((PARTS,))],
        compiler_params=pltpu.CompilerParams(vmem_limit_bytes=VMEM_COPY),
        name="write",
    )(mixed)


def solution(mesh):
    seq, batch = mesh.shape["seq"], mesh.shape["batch"]
    cores = 2
    A = math.gcd(seq, batch)
    B, X = seq // A, batch // cores
    grid = Mesh(mesh.devices.reshape(A, B, X, cores), ("a", "b", "x", "c"))
    seqs = ("a", "b")
    rows = P(("x", "c", "a", "b"), None)
    return jax.shard_map(
        functools.partial(local, (A, B, X)),
        mesh=grid,
        in_specs=(
            rows, rows, P(None, seqs), P(seqs), P(seqs, None), P(), P(None, seqs), P(seqs), P(None, seqs), P(seqs),
        ),
        out_specs=rows,
        check_vma=False,
    )
```
